128 devices in a mesh: sample: 4 (over x), gz: 32 (over z, y, core).
Axes of the slice: x: 4, y: 4, z: 4, core: 2. Of those that a mesh axis runs over, the one named last changes fastest.
Arguments:
- field_now: float32 [12, 64, 160, 256], P('sample', 'gz'), parts along dimension 0, may hold values from -6 to 6
- field_before: float32 [12, 64, 160, 256], P('sample', 'gz'), parts along dimension 0, may hold values from -6 to 6
- lame_lambda: float32 [64, 640, 256], P('gz', 'sample'), parts along dimension 1, may hold values from 0.5 to 1.5
- shear_modulus: float32 [64, 640, 256], P('gz', 'sample'), parts along dimension 1, may hold values from 0.5 to 1.5
- density: float32 [64, 640, 256], P('gz', 'sample'), parts along dimension 1, may hold values from 1 to 2
- source_field: float32 [12, 64, 160, 256], P('sample', 'gz'), parts along dimension 0, may hold values from -6 to 6
- wavelet: float32 [32], P('sample'), parts along dimension 0, may hold values from -4 to 4
- prior_mean: float32 [64, 640, 256], P('gz', 'sample'), parts along dimension 1, may hold values from 0.5 to 1.5
- steps_taken: float32 [16, 64, 160, 256], P('sample', 'gz'), parts along dimension 0
- grad_change: float32 [16, 64, 160, 256], P('sample', 'gz'), parts along dimension 0, as said below
Outputs:
- field_final: float32 [12, 64, 160, 256], P('sample', 'gz'), parts along dimension 0
- gradient: float32 [64, 640, 256], P('gz', 'sample'), parts along dimension 1
- direction: float32 [64, 640, 256], P('gz', 'sample'), parts along dimension 1
The draws below stay inside these ranges and needn't reach their ends.
There are 4 independent parts, one for each index of `sample`. The reference program is written for one: setup_inputs(seed, part) draws one part's arguments, and reference() takes and returns one part's arrays. A program takes and returns all parts, laid end to end along the dimension named above; each array names one. Nothing has to cross between parts.
Inputs may be any that keep to these rules, and one draw needn't show every extreme that they name: Each entry of grad_change is 0.5 to 2 times the matching entry of steps_taken.
All inputs are finite; a program needn't handle non-finite values.
Results may differ from the reference program's by a relative error of at most 0.0003.
Values sent between devices are 32-bit elements; how exact they have to be, the bound alone decides.
A program may use at most 64 MiB of HBM per device.

```python
import math
import jax
import jax.numpy as jnp
from jax import lax

NX = 160
NY = 256
STEPS = 8
PAIRS = 4
NZ = 64


def common_model(key):
    base = jax.random.fold_in(key, 11)
    keys = jax.random.split(base, 5)
    shape = (NZ, NX, NY)
    shear = jax.random.uniform(keys[0], shape, jnp.float32, 0.5, 1.5)
    prior = jax.random.uniform(keys[1], shape, jnp.float32, 0.5, 1.5)
    levels = 1.0 + 2.0 * jnp.arange(NZ, dtype=jnp.float32) / max(NZ - 1, 1)
    noise = jax.random.normal(keys[3], (PAIRS,) + shape, jnp.float32)
    weights = jax.random.uniform(keys[2], (PAIRS, 1, 1, 1), jnp.float32, 0.5, 2.0)
    updates = levels[None, :, None, None] * (weights * (shear - prior)[None] + 0.5 * noise)
    factors = jnp.exp(jax.random.uniform(keys[4], (PAIRS,) + shape, jnp.float32, -0.6931, 0.6931))
    changes = factors * updates
    return (shear, prior, updates, changes)


def draw_shear_modulus(key, part):
    return common_model(key)[0]


def draw_prior_mean(key, part):
    return common_model(key)[1]


def draw_steps_taken(key, part):
    return common_model(key)[2]


def draw_grad_change(key, part):
    return common_model(key)[3]


def shard_levels(rng, extent, cuts, low, top_value):
    def one(dim, shards_of):
        draws = jax.random.uniform(jax.random.fold_in(jax.random.fold_in(rng, 6), dim), (shards_of,), jnp.float32, low / len(cuts), top_value / len(cuts))
        return jnp.repeat(jnp.exp(draws), extent[dim] // shards_of).reshape((-1,) + (1,) * (len(extent) - dim - 1))

    level = one(*cuts[0])
    for cut in cuts[1:]:
        level = level * one(*cut)
    return level


def gaussian(key, extent, deviation, bound, pieces=(), kind=jnp.bfloat16):
    values = jax.random.normal(key, extent, jnp.float32) * deviation
    if len(pieces) > 0:
        values = shard_levels(key, extent, pieces, -0.22, 0.18) * values
    return jnp.clip(values, min=-bound, max=bound).astype(kind)


def setup_inputs(seed: int = 0, part: int = 0) -> dict:
    arg_keys = jax.random.split(jax.random.key(seed), 11)
    part_keys = jax.random.split(jax.random.fold_in(arg_keys[10], part), 11)
    field_now = gaussian(part_keys[0], (3, NZ, NX, NY), 1.0, 6.0, ((1, 32),), jnp.float32)
    field_before = gaussian(part_keys[1], (3, NZ, NX, NY), 1.0, 6.0, ((1, 32),), jnp.float32)
    lame_lambda = jnp.clip(0.5 + 1.0 * jax.random.uniform(part_keys[2], (NZ, NX, NY), jnp.float32) ** shard_levels(part_keys[2], (NZ, NX, NY), ((0, 32),), -0.2, 0.2), 0.5, 1.5)
    shear_modulus = draw_shear_modulus(jax.random.fold_in(jax.random.fold_in(arg_keys[10], part), 71), part)
    density = jnp.clip(jnp.exp(math.log(2.0) - 0.6931472 * jax.random.uniform(part_keys[4], (NZ, NX, NY), jnp.float32) ** shard_levels(part_keys[4], (NZ, NX, NY), ((0, 32),), -0.2, 0.2)), 1.0, 2.0)
    source_field = gaussian(part_keys[5], (3, NZ, NX, NY), 1.0, 6.0, ((1, 32),), jnp.float32)
    wavelet = gaussian(part_keys[6], (STEPS,), 1.0, 4.0, (), jnp.float32)
    prior_mean = draw_prior_mean(jax.random.fold_in(jax.random.fold_in(arg_keys[10], part), 71), part)
    steps_taken = draw_steps_taken(jax.random.fold_in(jax.random.fold_in(arg_keys[10], part), 71), part)
    grad_change = draw_grad_change(jax.random.fold_in(jax.random.fold_in(arg_keys[10], part), 71), part)
    return {"field_now": field_now, "field_before": field_before, "lame_lambda": lame_lambda, "shear_modulus": shear_modulus, "density": density, "source_field": source_field, "wavelet": wavelet, "prior_mean": prior_mean, "steps_taken": steps_taken, "grad_change": grad_change}


def shifted(padded, comp, offset):
    depth = padded.shape[1] - 2
    rows = padded.shape[2] - 2
    cols = padded.shape[3] - 2
    return lax.slice(padded[comp], (1 + offset[0], 1 + offset[1], 1 + offset[2]), (1 + offset[0] + depth, 1 + offset[1] + rows, 1 + offset[2] + cols))


def vec_add(first, second):
    return (first[0] + second[0], first[1] + second[1], first[2] + second[2])


def vec_neg(first):
    return (-first[0], -first[1], -first[2])


def operate(extended, lame_first, shear):
    padded = jnp.pad(extended, ((0, 0), (0, 0), (1, 1), (1, 1)))
    units = ((1, 0, 0), (0, 1, 0), (0, 0, 1))
    centre = (0, 0, 0)
    seconds = [[shifted(padded, comp, units[axis]) + shifted(padded, comp, vec_neg(units[axis])) - 2.0 * shifted(padded, comp, centre) for axis in range(3)] for comp in range(3)]

    def mixed(comp, first, second):
        plus_first = units[first]
        plus_second = units[second]
        return 0.25 * (shifted(padded, comp, vec_add(plus_first, plus_second)) - shifted(padded, comp, vec_add(plus_first, vec_neg(plus_second))) - shifted(padded, comp, vec_add(vec_neg(plus_first), plus_second)) + shifted(padded, comp, vec_neg(vec_add(plus_first, plus_second))))

    laplace = []
    elastic = []
    for comp in range(3):
        lap_comp = seconds[comp][0] + seconds[comp][1] + seconds[comp][2]
        grad_div = seconds[comp][comp]
        for other in range(3):
            if other != comp:
                grad_div = grad_div + mixed(other, comp, other)
        laplace.append(lap_comp)
        elastic.append((lame_first + shear) * grad_div + shear * lap_comp)
    return jnp.stack(elastic), jnp.stack(laplace)


def reference(field_now, field_before, lame_lambda, shear_modulus, density, source_field, wavelet, prior_mean, steps_taken, grad_change):
    coeff = 0.04 / density
    current = field_now
    earlier = field_before
    correlation = jnp.zeros(shear_modulus.shape, jnp.float32)
    for step in range(STEPS):
        extended = jnp.pad(current, ((0, 0), (1, 1), (0, 0), (0, 0)))
        elastic, laplace = operate(extended, lame_lambda, shear_modulus)
        correlation = correlation + jnp.sum(current * laplace, axis=0)
        nxt = 2.0 * current - earlier + coeff * (elastic + wavelet[step] * source_field)
        earlier = current
        current = nxt
    gradient = (shear_modulus - prior_mean) + 0.02 * correlation
    curv = [jnp.sum(steps_taken[i] * grad_change[i]) for i in range(PAIRS)]
    query = gradient
    alphas = [None] * PAIRS
    for i in reversed(range(PAIRS)):
        alphas[i] = jnp.sum(steps_taken[i] * query) / curv[i]
        query = query - alphas[i] * grad_change[i]
    newest = grad_change[PAIRS - 1]
    result = (curv[PAIRS - 1] / jnp.sum(newest * newest)) * query
    for i in range(PAIRS):
        beta = jnp.sum(grad_change[i] * result) / curv[i]
        result = result + (alphas[i] - beta) * steps_taken[i]
    return current, gradient, -result
```

```python
import jax
import jax.numpy as jnp
from jax import lax
from jax.experimental import pallas as pl
from jax.experimental.pallas import tpu as pltpu
from jax.sharding import PartitionSpec as P

STEPS = 8
PAIRS = 4
ROWS = 16
PAD = 8
LANES = 128
MESH = pl.DeviceIdType.MESH


def kernel(
    now, before, lame, shear, density, source, wavelet, prior, steps, changes,
    out_field, out_gradient, out_direction,
    field, halo, first_coef, second_coef, force, grad, s_vec, y_vec, spare, row, rows,
    send_sem, recv_sem, load_sem, store_sem, sum_send, sum_recv,
):
    me = lax.axis_index("gz")
    count = lax.axis_size("gz")
    nx = first_coef.shape[2]
    chunks = nx // ROWS
    padded = nx + 2 * PAD
    zero = jnp.zeros((8, LANES), jnp.float32)
    lane = lax.broadcasted_iota(jnp.int32, (8, LANES), 1)
    row_lane = lax.broadcasted_iota(jnp.int32, (1, LANES), 1)
    at_start = lane == 0
    at_end = lane == LANES - 1
    exists = (me > 0, me < count - 1)
    beside = (jnp.maximum(me - 1, 0), jnp.minimum(me + 1, count - 1))

    inner = pl.ds(PAD, nx)
    loads = []

    def load(src, dst_of):
        for h in range(2):
            copy = pltpu.make_async_copy(
                src.at[..., pl.ds(h * LANES, LANES)], dst_of(h), load_sem.at[len(loads)]
            )
            copy.start()
            loads.append(copy)

    load(now, lambda h: field.at[0, :, :, h, inner, :])
    load(lame, lambda h: first_coef.at[:, h])
    load(shear, lambda h: second_coef.at[:, h])
    load(density, lambda h: spare.at[:, h])
    load(source, lambda h: force.at[:, :, h])
    load(prior, lambda h: grad.at[:, h])
    load(before, lambda h: field.at[1, :, :, h, inner, :])
    load(steps, lambda h: s_vec.at[:, :, h])
    load(changes, lambda h: y_vec.at[:, :, h])

    barrier = pltpu.get_barrier_semaphore()

    def greet(k, carry):
        pl.semaphore_signal(
            barrier, inc=1, device_id={"gz": lax.rem(me + k, count)}, device_id_type=MESH
        )
        return carry

    for par in range(2):
        for c in range(3):
            for d in range(2):
                for h in range(2):
                    for edge in (0, padded - PAD):
                        field[par, c, d, h, edge : edge + 8, :] = zero
                        halo[par, d, c, h, edge : edge + 8, :] = zero
    for d in range(2):

        @pl.when(jnp.logical_not(exists[d]))
        def _():
            def clear(i, carry):
                at = pl.ds(pl.multiple_of(i * 8, 8), 8)
                for par in range(2):
                    for c in range(3):
                        for h in range(2):
                            halo[par, d, c, h, at, :] = zero
                return carry

            lax.fori_loop(0, padded // 8, clear, 0)

    lax.fori_loop(1, count, greet, 0)
    pl.semaphore_wait(barrier, count - 1)

    def outgoing(par, d, j):
        at = pl.ds(pl.multiple_of(PAD + j * ROWS, 8), ROWS)
        return pltpu.make_async_remote_copy(
            src_ref=field.at[par, :, d, :, at, :],
            dst_ref=halo.at[par, 1 - d, :, :, at, :],
            send_sem=send_sem.at[par, d, j],
            recv_sem=recv_sem.at[par, 1 - d, j],
            device_id={"gz": beside[d]},
            device_id_type=MESH,
        )

    def incoming(par, d, j):
        at = pl.ds(pl.multiple_of(PAD + j * ROWS, 8), ROWS)
        return pltpu.make_async_remote_copy(
            src_ref=field.at[par, :, d, :, at, :],
            dst_ref=halo.at[par, d, :, :, at, :],
            send_sem=send_sem.at[par, d, j],
            recv_sem=recv_sem.at[par, d, j],
            device_id={"gz": beside[d]},
            device_id_type=MESH,
        )

    def send(par, j):
        for d in range(2):
            pl.when(exists[d])(lambda d=d: outgoing(par, d, j).start())

    def wait_sent(par, j):
        for d in range(2):
            pl.when(exists[d])(lambda d=d: outgoing(par, d, j).wait_send())

    def wait_halo(par, j):
        for d in range(2):
            pl.when(exists[d])(lambda d=d: incoming(par, d, j).wait_recv())

    for copy in loads[:2]:
        copy.wait()

    def first_send(j, carry):
        send(0, j)
        return carry

    lax.fori_loop(0, chunks, first_send, 0)

    for copy in loads[2:12]:
        copy.wait()

    def prepare(i, carry):
        at = pl.ds(pl.multiple_of(i * 8, 8), 8)
        for p in range(2):
            for h in range(2):
                mu = second_coef[p, h, at, :]
                coeff = 0.04 / spare[p, h, at, :]
                first_coef[p, h, at, :] = 0.25 * coeff * (first_coef[p, h, at, :] + mu)
                second_coef[p, h, at, :] = coeff * mu
                grad[p, h, at, :] = mu - grad[p, h, at, :]
                for c in range(3):
                    force[c, p, h, at, :] = coeff * force[c, p, h, at, :]
        return carry

    lax.fori_loop(0, nx // 8, prepare, 0)

    for copy in loads[12:]:
        copy.wait()
    wanted = [("sy", i, j) for i in range(PAIRS) for j in range(i, PAIRS)]
    wanted += [("yy", i, j) for i in range(PAIRS) for j in range(i, PAIRS)]

    def gram(i, sums):
        at = pl.ds(pl.multiple_of(i * 8, 8), 8)
        sums = list(sums)
        for p in range(2):
            for h in range(2):
                s = [s_vec[k, p, h, at, :] for k in range(PAIRS)]
                y = [y_vec[k, p, h, at, :] for k in range(PAIRS)]
                for w, (kind, a, b) in enumerate(wanted):
                    sums[w] = sums[w] + (s[a] if kind == "sy" else y[a]) * y[b]
        return tuple(sums)

    def total_of(x):
        return jnp.sum(jnp.sum(x, axis=0, keepdims=True), axis=1, keepdims=True)

    sums = lax.fori_loop(0, nx // 8, gram, (zero,) * len(wanted))
    gram_row = jnp.zeros((1, LANES), jnp.float32)
    for w, x in enumerate(sums):
        gram_row = jnp.where(row_lane == 2 * PAIRS + w, total_of(x), gram_row)
    row[...] = gram_row

    def along_y(v):
        back = [pltpu.roll(x, 1, 1) for x in v]
        ahead = [pltpu.roll(x, LANES - 1, 1) for x in v]
        plus = (jnp.where(at_end, ahead[1], ahead[0]), jnp.where(at_end, 0.0, ahead[1]))
        minus = (jnp.where(at_start, 0.0, back[0]), jnp.where(at_start, back[0], back[1]))
        return plus, minus

    def add(a, b):
        return (a[0] + b[0], a[1] + b[1])

    def sub(a, b):
        return (a[0] - b[0], a[1] - b[1])

    def block(cur, nxt, amplitude, base):
        at = pl.ds(base, 8)

        def rows_of(c, z, offset):
            from_row = pl.ds(base + PAD + offset, 8)
            if z in (-1, 2):
                return tuple(halo[cur, 0 if z < 0 else 1, c, h, from_row, :] for h in range(2))
            return tuple(field[cur, c, z, h, from_row, :] for h in range(2))

        u = {(c, z): rows_of(c, z, 0) for c in range(3) for z in (-1, 0, 1, 2)}
        up = {}
        down = {}
        for c in range(3):
            for z in (-1, 0, 1, 2) if c < 2 else (0, 1):
                up[c, z] = rows_of(c, z, 1)
                down[c, z] = rows_of(c, z, -1)
        dx = {key: sub(up[key], down[key]) for key in up}
        dy2 = {}
        sy = {}
        for z in (-1, 0, 1, 2):
            plus, minus = along_y(u[2, z])
            dy2[z] = sub(plus, minus)
            if z in (0, 1):
                sy[2, z] = add(plus, minus)
        mix0 = {z: add(dx[1, z], dy2[z]) for z in (-1, 0, 1, 2)}
        grads = []
        for z in range(2):
            for c in range(2):
                sy[c, z] = add(*along_y(u[c, z]))
            dz0 = sub(u[0, z + 1], u[0, z - 1])
            cross = [
                sub(mix0[z + 1], mix0[z - 1]),
                add(sub(dx[0, z + 1], dx[0, z - 1]), sub(*along_y(dx[2, z]))),
                sub(*along_y(add(dz0, dx[1, z]))),
            ]
            work = [None, None]
            for c in range(3):
                sz = add(u[c, z + 1], u[c, z - 1])
                sx = add(up[c, z], down[c, z])
                own = (sz, sx, sy[c, z])[c]
                for h in range(2):
                    centre = u[c, z][h]
                    twice = centre + centre
                    laplace = sz[h] + sx[h] + sy[c, z][h] - 6.0 * centre
                    div = 4.0 * (own[h] - twice) + cross[c][h]
                    field[nxt, c, z, h, pl.ds(base + PAD, 8), :] = (
                        twice
                        - field[nxt, c, z, h, pl.ds(base + PAD, 8), :]
                        + first_coef[z, h, at, :] * div
                        + second_coef[z, h, at, :] * laplace
                        + amplitude * force[c, z, h, at, :]
                    )
                    term = centre * laplace
                    work[h] = term if work[h] is None else work[h] + term
            for h in range(2):
                new = grad[z, h, at, :] + 0.02 * work[h]
                grad[z, h, at, :] = new
                grads.append((z, h, new))
        return grads

    def step(n, carry):
        cur = lax.rem(n, 2)
        nxt = 1 - cur
        amplitude = wavelet[n]
        wait_halo(cur, 0)

        def chunk(j, inside):
            pl.when(j + 1 < chunks)(lambda: wait_halo(cur, j + 1))
            pl.when(n >= 1)(lambda: wait_sent(nxt, j))
            for b in range(ROWS // 8):
                block(cur, nxt, amplitude, pl.multiple_of(j * ROWS + b * 8, 8))
            send(nxt, j)
            return inside

        return lax.fori_loop(0, chunks, chunk, carry)

    lax.fori_loop(0, STEPS - 1, step, 0)

    cur, nxt = (STEPS - 1) % 2, STEPS % 2
    wait_halo(cur, 0)

    def last_chunk(j, sums):
        pl.when(j + 1 < chunks)(lambda: wait_halo(cur, j + 1))
        wait_sent(nxt, j)
        sums = list(sums)
        for b in range(ROWS // 8):
            base = pl.multiple_of(j * ROWS + b * 8, 8)
            for z, h, g in block(cur, nxt, wavelet[STEPS - 1], base):
                for k in range(PAIRS):
                    sums[k] = sums[k] + s_vec[k, z, h, pl.ds(base, 8), :] * g
                    sums[PAIRS + k] = sums[PAIRS + k] + y_vec[k, z, h, pl.ds(base, 8), :] * g
        return tuple(sums)

    sums = lax.fori_loop(0, chunks, last_chunk, (zero,) * (2 * PAIRS))

    mine = row[...]
    for w, x in enumerate(sums):
        mine = jnp.where(row_lane == w, total_of(x), mine)
    row[...] = mine

    def tell(k, carry):
        pltpu.make_async_remote_copy(
            src_ref=row,
            dst_ref=rows.at[k - 1],
            send_sem=sum_send.at[0],
            recv_sem=sum_recv.at[0],
            device_id={"gz": lax.rem(me + k, count)},
            device_id_type=MESH,
        ).start()
        return carry

    lax.fori_loop(1, count, tell, 0)

    stores = []
    for h in range(2):
        half = pl.ds(h * LANES, LANES)
        stores.append(
            pltpu.make_async_copy(
                field.at[nxt, :, :, h, inner, :], out_field.at[..., half], store_sem.at[h]
            )
        )
        stores.append(
            pltpu.make_async_copy(grad.at[:, h], out_gradient.at[..., half], store_sem.at[2 + h])
        )
    for copy in stores:
        copy.start()

    def last_sent(j, carry):
        wait_sent(cur, j)
        return carry

    lax.fori_loop(0, chunks, last_sent, 0)

    everyone = pltpu.make_async_remote_copy(
        src_ref=rows,
        dst_ref=rows,
        send_sem=sum_send.at[0],
        recv_sem=sum_recv.at[0],
        device_id={"gz": lax.rem(me + 1, count)},
        device_id_type=MESH,
    )
    everyone.wait_send()
    everyone.wait_recv()
    total = row[...] + jnp.sum(rows[...], axis=0)

    def value(k):
        return jnp.sum(jnp.where(row_lane == k, total, 0.0), axis=1, keepdims=True)

    sg = [value(k) for k in range(PAIRS)]
    yg = [value(PAIRS + k) for k in range(PAIRS)]
    pair = {}
    for w, (kind, a, b) in enumerate(wanted):
        pair[kind, a, b] = value(2 * PAIRS + w)
        if kind == "yy":
            pair[kind, b, a] = pair[kind, a, b]
    alphas = [None] * PAIRS
    for i in reversed(range(PAIRS)):
        dot = sg[i]
        for j in range(i + 1, PAIRS):
            dot = dot - alphas[j] * pair["sy", i, j]
        alphas[i] = dot / pair["sy", i, i]
    gamma = pair["sy", PAIRS - 1, PAIRS - 1] / pair["yy", PAIRS - 1, PAIRS - 1]
    extra = []
    for i in range(PAIRS):
        dot = yg[i]
        for j in range(PAIRS):
            dot = dot - alphas[j] * pair["yy", i, j]
        dot = gamma * dot
        for j in range(i):
            dot = dot + extra[j] * pair["sy", j, i]
        extra.append(alphas[i] - dot / pair["sy", i, i])

    def wide(x):
        return jnp.broadcast_to(x, (8, LANES))

    of_g = wide(-gamma)
    of_y = [wide(gamma * alphas[i]) for i in range(PAIRS)]
    of_s = [wide(-extra[i]) for i in range(PAIRS)]

    def combine(i, carry):
        at = pl.ds(pl.multiple_of(i * 8, 8), 8)
        for p in range(2):
            for h in range(2):
                out = of_g * grad[p, h, at, :]
                for k in range(PAIRS):
                    out = out + of_y[k] * y_vec[k, p, h, at, :] + of_s[k] * s_vec[k, p, h, at, :]
                spare[p, h, at, :] = out
        return carry

    lax.fori_loop(0, nx // 8, combine, 0)
    for h in range(2):
        copy = pltpu.make_async_copy(
            spare.at[:, h], out_direction.at[..., pl.ds(h * LANES, LANES)], store_sem.at[4 + h]
        )
        copy.start()
        stores.append(copy)
    for copy in stores:
        copy.wait()


def on_device(*args):
    now = args[0]
    lame = args[2]
    nx = now.shape[2]
    count = lax.axis_size("gz")
    padded = nx + 2 * PAD
    chunks = nx // ROWS
    f32 = jnp.float32
    anywhere = pl.BlockSpec(memory_space=pl.ANY)
    in_specs = [anywhere] * 10
    in_specs[6] = pl.BlockSpec(memory_space=pltpu.SMEM)
    plane = (2, 2, nx, LANES)
    return pl.pallas_call(
        kernel,
        out_shape=(
            jax.ShapeDtypeStruct(now.shape, f32),
            jax.ShapeDtypeStruct(lame.shape, f32),
            jax.ShapeDtypeStruct(lame.shape, f32),
        ),
        in_specs=in_specs,
        out_specs=(anywhere,) * 3,
        scratch_shapes=[
            pltpu.VMEM((2, 3, 2, 2, padded, LANES), f32),
            pltpu.VMEM((2, 2, 3, 2, padded, LANES), f32),
            pltpu.VMEM(plane, f32),
            pltpu.VMEM(plane, f32),
            pltpu.VMEM((3, *plane), f32),
            pltpu.VMEM(plane, f32),
            pltpu.VMEM((PAIRS, *plane), f32),
            pltpu.VMEM((PAIRS, *plane), f32),
            pltpu.VMEM(plane, f32),
            pltpu.VMEM((1, LANES), f32),
            pltpu.VMEM((count - 1, 1, LANES), f32),
            pltpu.SemaphoreType.DMA((2, 2, chunks)),
            pltpu.SemaphoreType.DMA((2, 2, chunks)),
            pltpu.SemaphoreType.DMA((18,)),
            pltpu.SemaphoreType.DMA((6,)),
            pltpu.SemaphoreType.DMA((1,)),
            pltpu.SemaphoreType.DMA((1,)),
        ],
        compiler_params=pltpu.CompilerParams(
            collective_id=0, has_side_effects=True, vmem_limit_bytes=60 * 1024 * 1024
        ),
        name="leapfrog",
    )(*args)


def solution(mesh):
    placed = (
        P("sample", "gz", None, None),
        P("sample", "gz", None, None),
        P("gz", "sample", None),
        P("gz", "sample", None),
        P("gz", "sample", None),
        P("sample", "gz", None, None),
        P("sample"),
        P("gz", "sample", None),
        P("sample", "gz", None, None),
        P("sample", "gz", None, None),
    )
    return jax.shard_map(
        on_device,
        mesh=mesh,
        in_specs=placed,
        out_specs=(P("sample", "gz", None, None), P("gz", "sample", None), P("gz", "sample", None)),
        check_vma=False,
    )
```

```python
import jax
import jax.numpy as jnp
from jax import lax
from jax.experimental import pallas as pl
from jax.experimental.pallas import tpu as pltpu
from jax.sharding import PartitionSpec as P

STEPS = 8
PAIRS = 4
ROWS = 16
PAD = 8
LANES = 128
MESH = pl.DeviceIdType.MESH


def kernel(
    now, before, lame, shear, density, source, wave, prior, steps, changes,
    final, grad, spare,
    wavelet, field, halo, first_coef, second_coef, force, s_vec, y_vec, row, rows,
    send_sem, recv_sem, load_sem, hello_sem, sum_send, sum_recv,
):
    me = lax.axis_index("gz")
    count = lax.axis_size("gz")
    nx = first_coef.shape[2]
    chunks = nx // ROWS
    padded = nx + 2 * PAD
    zero = jnp.zeros((8, LANES), jnp.float32)
    lane = lax.broadcasted_iota(jnp.int32, (8, LANES), 1)
    row_lane = lax.broadcasted_iota(jnp.int32, (1, LANES), 1)
    at_start = lane == 0
    at_end = lane == LANES - 1
    exists = (me > 0, me < count - 1)
    beside = (jnp.maximum(me - 1, 0), jnp.minimum(me + 1, count - 1))

    inner = pl.ds(PAD, nx)
    loads = []

    def load(src, dst_of):
        for h in range(2):
            copy = pltpu.make_async_copy(
                src.at[..., pl.ds(h * LANES, LANES)], dst_of(h), load_sem.at[len(loads)]
            )
            copy.start()
            loads.append(copy)

    load(now, lambda h: field.at[0, :, :, h, inner, :])
    wave_copy = pltpu.make_async_copy(wave, wavelet, load_sem.at[18])
    wave_copy.start()
    load(lame, lambda h: first_coef.at[:, h])
    load(shear, lambda h: second_coef.at[:, h])
    load(density, lambda h: spare.at[:, h])
    load(source, lambda h: force.at[:, :, h])
    load(prior, lambda h: grad.at[:, h])
    load(before, lambda h: field.at[1, :, :, h, inner, :])
    load(steps, lambda h: s_vec.at[:, :, h])
    load(changes, lambda h: y_vec.at[:, :, h])

    barrier = pltpu.get_barrier_semaphore()
    for d in range(2):

        @pl.when(exists[d])
        def _():
            pl.semaphore_signal(barrier, inc=1, device_id={"gz": beside[d]}, device_id_type=MESH)

    for par in range(2):
        for c in range(3):
            for d in range(2):
                for h in range(2):
                    for edge in (0, padded - PAD):
                        field[par, c, d, h, edge : edge + 8, :] = zero
                        halo[par, d, c, h, edge : edge + 8, :] = zero
    for d in range(2):

        @pl.when(jnp.logical_not(exists[d]))
        def _():
            def clear(i, carry):
                at = pl.ds(pl.multiple_of(i * 8, 8), 8)
                for par in range(2):
                    for c in range(3):
                        for h in range(2):
                            halo[par, d, c, h, at, :] = zero
                return carry

            lax.fori_loop(0, padded // 8, clear, 0)

    pl.semaphore_wait(barrier, jnp.where(me > 0, 1, 0) + jnp.where(me < count - 1, 1, 0))

    def outgoing(par, d, j):
        at = pl.ds(pl.multiple_of(PAD + j * ROWS, 8), ROWS)
        return pltpu.make_async_remote_copy(
            src_ref=field.at[par, :, d, :, at, :],
            dst_ref=halo.at[par, 1 - d, :, :, at, :],
            send_sem=send_sem.at[par, d, j],
            recv_sem=recv_sem.at[par, 1 - d, j],
            device_id={"gz": beside[d]},
            device_id_type=MESH,
        )

    def incoming(par, d, j):
        at = pl.ds(pl.multiple_of(PAD + j * ROWS, 8), ROWS)
        return pltpu.make_async_remote_copy(
            src_ref=field.at[par, :, d, :, at, :],
            dst_ref=halo.at[par, d, :, :, at, :],
            send_sem=send_sem.at[par, d, j],
            recv_sem=recv_sem.at[par, d, j],
            device_id={"gz": beside[d]},
            device_id_type=MESH,
        )

    def send(par, j):
        for d in range(2):
            pl.when(exists[d])(lambda d=d: outgoing(par, d, j).start())

    def wait_sent(par, j):
        for d in range(2):
            pl.when(exists[d])(lambda d=d: outgoing(par, d, j).wait_send())

    def wait_halo(par, j):
        for d in range(2):
            pl.when(exists[d])(lambda d=d: incoming(par, d, j).wait_recv())

    rounds = []
    while 4 << len(rounds) < count:
        rounds.append(4 << len(rounds))

    def far(r, d):
        return me + rounds[r] if d else me - rounds[r]

    def within(r, d):
        return far(r, d) < count if d else far(r, d) >= 0

    def tell_far(r):
        for d in range(2):

            @pl.when(within(r, d))
            def _():
                pl.semaphore_signal(
                    hello_sem.at[r, 1 - d], inc=1, device_id={"gz": far(r, d)}, device_id_type=MESH
                )

    def hear_far(r):
        for d in range(2):

            @pl.when(within(r, d))
            def _():
                pl.semaphore_wait(hello_sem.at[r, d], 1)

    def acquaint(n):
        for r in range(len(rounds) + 1):

            @pl.when(n == 2 + r)
            def _():
                if r > 0:
                    hear_far(r - 1)
                if r < len(rounds):
                    tell_far(r)

    for copy in loads[:2]:
        copy.wait()

    def first_send(j, carry):
        send(0, j)
        return carry

    lax.fori_loop(0, chunks, first_send, 0)

    wave_copy.wait()
    for copy in loads[2:12]:
        copy.wait()

    def prepare(i, carry):
        at = pl.ds(pl.multiple_of(i * 8, 8), 8)
        for p in range(2):
            for h in range(2):
                mu = second_coef[p, h, at, :]
                coeff = 0.04 / spare[p, h, at, :]
                first_coef[p, h, at, :] = 0.25 * coeff * (first_coef[p, h, at, :] + mu)
                second_coef[p, h, at, :] = coeff * mu
                grad[p, h, at, :] = mu - grad[p, h, at, :]
                for c in range(3):
                    force[c, p, h, at, :] = coeff * force[c, p, h, at, :]
        return carry

    lax.fori_loop(0, nx // 8, prepare, 0)

    for copy in loads[12:]:
        copy.wait()
    wanted = [("sy", i, j) for i in range(PAIRS) for j in range(i, PAIRS)]
    wanted += [("yy", i, j) for i in range(PAIRS) for j in range(i, PAIRS)]

    def gram(i, sums):
        at = pl.ds(pl.multiple_of(i * 8, 8), 8)
        sums = list(sums)
        for p in range(2):
            for h in range(2):
                s = [s_vec[k, p, h, at, :] for k in range(PAIRS)]
                y = [y_vec[k, p, h, at, :] for k in range(PAIRS)]
                for w, (kind, a, b) in enumerate(wanted):
                    sums[w] = sums[w] + (s[a] if kind == "sy" else y[a]) * y[b]
        return tuple(sums)

    def total_of(x):
        return jnp.sum(jnp.sum(x, axis=0, keepdims=True), axis=1, keepdims=True)

    sums = lax.fori_loop(0, nx // 8, gram, (zero,) * len(wanted))
    gram_row = jnp.zeros((1, LANES), jnp.float32)
    for w, x in enumerate(sums):
        gram_row = jnp.where(row_lane == 2 * PAIRS + w, total_of(x), gram_row)
    row[...] = gram_row

    def along_y(v):
        back = [pltpu.roll(x, 1, 1) for x in v]
        ahead = [pltpu.roll(x, LANES - 1, 1) for x in v]
        plus = (jnp.where(at_end, ahead[1], ahead[0]), jnp.where(at_end, 0.0, ahead[1]))
        minus = (jnp.where(at_start, 0.0, back[0]), jnp.where(at_start, back[0], back[1]))
        return plus, minus

    def add(a, b):
        return (a[0] + b[0], a[1] + b[1])

    def sub(a, b):
        return (a[0] - b[0], a[1] - b[1])

    def block(cur, nxt, amplitude, base, out=None):
        at = pl.ds(base, 8)

        def rows_of(c, z, offset):
            from_row = pl.ds(base + PAD + offset, 8)
            if z in (-1, 2):
                return tuple(halo[cur, 0 if z < 0 else 1, c, h, from_row, :] for h in range(2))
            return tuple(field[cur, c, z, h, from_row, :] for h in range(2))

        u = {(c, z): rows_of(c, z, 0) for c in range(3) for z in (-1, 0, 1, 2)}
        up = {}
        down = {}
        for c in range(3):
            for z in (-1, 0, 1, 2) if c < 2 else (0, 1):
                up[c, z] = rows_of(c, z, 1)
                down[c, z] = rows_of(c, z, -1)
        dx = {key: sub(up[key], down[key]) for key in up}
        dy2 = {}
        sy = {}
        for z in (-1, 0, 1, 2):
            plus, minus = along_y(u[2, z])
            dy2[z] = sub(plus, minus)
            if z in (0, 1):
                sy[2, z] = add(plus, minus)
        mix0 = {z: add(dx[1, z], dy2[z]) for z in (-1, 0, 1, 2)}
        grads = []
        for z in range(2):
            for c in range(2):
                sy[c, z] = add(*along_y(u[c, z]))
            dz0 = sub(u[0, z + 1], u[0, z - 1])
            cross = [
                sub(mix0[z + 1], mix0[z - 1]),
                add(sub(dx[0, z + 1], dx[0, z - 1]), sub(*along_y(dx[2, z]))),
                sub(*along_y(add(dz0, dx[1, z]))),
            ]
            work = [None, None]
            for c in range(3):
                sz = add(u[c, z + 1], u[c, z - 1])
                sx = add(up[c, z], down[c, z])
                own = (sz, sx, sy[c, z])[c]
                for h in range(2):
                    centre = u[c, z][h]
                    twice = centre + centre
                    laplace = sz[h] + sx[h] + sy[c, z][h] - 6.0 * centre
                    div = 4.0 * (own[h] - twice) + cross[c][h]
                    new = (
                        twice
                        - field[nxt, c, z, h, pl.ds(base + PAD, 8), :]
                        + first_coef[z, h, at, :] * div
                        + second_coef[z, h, at, :] * laplace
                        + amplitude * force[c, z, h, at, :]
                    )
                    if out is None:
                        field[nxt, c, z, h, pl.ds(base + PAD, 8), :] = new
                    else:
                        out[c, z, h, at, :] = new
                    term = centre * laplace
                    work[h] = term if work[h] is None else work[h] + term
            for h in range(2):
                new = grad[z, h, at, :] + 0.02 * work[h]
                grad[z, h, at, :] = new
                grads.append((z, h, new))
        return grads

    def step(n, carry):
        cur = lax.rem(n, 2)
        nxt = 1 - cur
        amplitude = wavelet[n]
        wait_halo(cur, 0)
        acquaint(n)

        def chunk(j, inside):
            pl.when(j + 1 < chunks)(lambda: wait_halo(cur, j + 1))
            pl.when(n >= 1)(lambda: wait_sent(nxt, j))
            for b in range(ROWS // 8):
                block(cur, nxt, amplitude, pl.multiple_of(j * ROWS + b * 8, 8))
            send(nxt, j)
            return inside

        return lax.fori_loop(0, chunks, chunk, carry)

    lax.fori_loop(0, STEPS - 1, step, 0)

    cur, nxt = (STEPS - 1) % 2, STEPS % 2
    wait_halo(cur, 0)

    def last_chunk(j, sums):
        pl.when(j + 1 < chunks)(lambda: wait_halo(cur, j + 1))
        sums = list(sums)
        for b in range(ROWS // 8):
            base = pl.multiple_of(j * ROWS + b * 8, 8)
            for z, h, g in block(cur, nxt, wavelet[STEPS - 1], base, final):
                for k in range(PAIRS):
                    sums[k] = sums[k] + s_vec[k, z, h, pl.ds(base, 8), :] * g
                    sums[PAIRS + k] = sums[PAIRS + k] + y_vec[k, z, h, pl.ds(base, 8), :] * g
        return tuple(sums)

    sums = lax.fori_loop(0, chunks, last_chunk, (zero,) * (2 * PAIRS))

    mine = row[...]
    for w, x in enumerate(sums):
        mine = jnp.where(row_lane == w, total_of(x), mine)
    row[...] = mine

    spots = [(k,) for k in range(1, count)]
    if count == 32:
        spots = [(a, b, c) for a in range(4) for b in range(4) for c in range(2)][1:]
        spots.sort(key=lambda t: -min(t[0], 4 - t[0]) - min(t[1], 4 - t[1]) - 0.1 * t[2])
    core, along, slow = lax.rem(me, 2), lax.rem(me // 2, 4), me // 8
    for k, spot in enumerate(spots):
        if count == 32:
            other = lax.rem(slow + spot[0], 4) * 8 + lax.rem(along + spot[1], 4) * 2
            other = other + (1 - core if spot[2] else core)
        else:
            other = lax.rem(me + spot[0], count)
        pltpu.make_async_remote_copy(
            src_ref=row,
            dst_ref=rows.at[k],
            send_sem=sum_send.at[0],
            recv_sem=sum_recv.at[0],
            device_id={"gz": other},
            device_id_type=MESH,
        ).start()

    def last_sent(j, carry):
        wait_sent(nxt, j)
        wait_sent(cur, j)
        return carry

    lax.fori_loop(0, chunks, last_sent, 0)

    everyone = pltpu.make_async_remote_copy(
        src_ref=rows,
        dst_ref=rows,
        send_sem=sum_send.at[0],
        recv_sem=sum_recv.at[0],
        device_id={"gz": lax.rem(me + 1, count)},
        device_id_type=MESH,
    )
    everyone.wait_send()
    everyone.wait_recv()
    total = row[...] + jnp.sum(rows[...], axis=0)

    def value(k):
        return jnp.sum(jnp.where(row_lane == k, total, 0.0), axis=1, keepdims=True)

    sg = [value(k) for k in range(PAIRS)]
    yg = [value(PAIRS + k) for k in range(PAIRS)]
    pair = {}
    for w, (kind, a, b) in enumerate(wanted):
        pair[kind, a, b] = value(2 * PAIRS + w)
        if kind == "yy":
            pair[kind, b, a] = pair[kind, a, b]
    alphas = [None] * PAIRS
    for i in reversed(range(PAIRS)):
        dot = sg[i]
        for j in range(i + 1, PAIRS):
            dot = dot - alphas[j] * pair["sy", i, j]
        alphas[i] = dot / pair["sy", i, i]
    gamma = pair["sy", PAIRS - 1, PAIRS - 1] / pair["yy", PAIRS - 1, PAIRS - 1]
    extra = []
    for i in range(PAIRS):
        dot = yg[i]
        for j in range(PAIRS):
            dot = dot - alphas[j] * pair["yy", i, j]
        dot = gamma * dot
        for j in range(i):
            dot = dot + extra[j] * pair["sy", j, i]
        extra.append(alphas[i] - dot / pair["sy", i, i])

    def wide(x):
        return jnp.broadcast_to(x, (8, LANES))

    of_g = wide(-gamma)
    of_y = [wide(gamma * alphas[i]) for i in range(PAIRS)]
    of_s = [wide(-extra[i]) for i in range(PAIRS)]

    def combine(i, carry):
        at = pl.ds(pl.multiple_of(i * 8, 8), 8)
        for p in range(2):
            for h in range(2):
                out = of_g * grad[p, h, at, :]
                for k in range(PAIRS):
                    out = out + of_y[k] * y_vec[k, p, h, at, :] + of_s[k] * s_vec[k, p, h, at, :]
                spare[p, h, at, :] = out
        return carry

    lax.fori_loop(0, nx // 8, combine, 0)


def write_out(final, grad, spare, out_field, out_gradient, out_direction, sem):
    copies = []
    for h in range(2):
        half = pl.ds(h * LANES, LANES)
        for src, dst in (
            (final.at[:, :, h], out_field),
            (grad.at[:, h], out_gradient),
            (spare.at[:, h], out_direction),
        ):
            copies.append(
                pltpu.make_async_copy(src, dst.at[..., half], sem.at[len(copies)])
            )
    for copy in copies:
        copy.start()
    for copy in copies:
        copy.wait()


def on_device(*args):
    now = args[0]
    lame = args[2]
    nx = now.shape[2]
    count = lax.axis_size("gz")
    padded = nx + 2 * PAD
    chunks = nx // ROWS
    f32 = jnp.float32
    hbm = pl.BlockSpec(memory_space=pltpu.HBM)
    vmem = pl.BlockSpec(memory_space=pltpu.VMEM)
    in_specs = [hbm] * 10
    plane = (2, 2, nx, LANES)
    halves = pl.pallas_call(
        kernel,
        out_shape=(
            jax.ShapeDtypeStruct((3, *plane), f32),
            jax.ShapeDtypeStruct(plane, f32),
            jax.ShapeDtypeStruct(plane, f32),
        ),
        in_specs=in_specs,
        out_specs=(vmem,) * 3,
        scratch_shapes=[
            pltpu.SMEM((STEPS,), f32),
            pltpu.VMEM((2, 3, 2, 2, padded, LANES), f32),
            pltpu.VMEM((2, 2, 3, 2, padded, LANES), f32),
            pltpu.VMEM(plane, f32),
            pltpu.VMEM(plane, f32),
            pltpu.VMEM((3, *plane), f32),
            pltpu.VMEM((PAIRS, *plane), f32),
            pltpu.VMEM((PAIRS, *plane), f32),
            pltpu.VMEM((1, LANES), f32),
            pltpu.VMEM((count - 1, 1, LANES), f32),
            pltpu.SemaphoreType.DMA((2, 2, chunks)),
            pltpu.SemaphoreType.DMA((2, 2, chunks)),
            pltpu.SemaphoreType.DMA((19,)),
            pltpu.SemaphoreType.REGULAR((3, 2)),
            pltpu.SemaphoreType.DMA((1,)),
            pltpu.SemaphoreType.DMA((1,)),
        ],
        compiler_params=pltpu.CompilerParams(
            collective_id=0, has_side_effects=True, vmem_limit_bytes=20 * 1024 * 1024
        ),
        name="leapfrog",
    )(*[pltpu.with_memory_space_constraint(x, pltpu.HBM) for x in args])
    return pl.pallas_call(
        write_out,
        out_shape=(
            jax.ShapeDtypeStruct(now.shape, f32),
            jax.ShapeDtypeStruct(lame.shape, f32),
            jax.ShapeDtypeStruct(lame.shape, f32),
        ),
        in_specs=[vmem] * 3,
        out_specs=(hbm,) * 3,
        scratch_shapes=[pltpu.SemaphoreType.DMA((6,))],
        compiler_params=pltpu.CompilerParams(vmem_limit_bytes=8 * 1024 * 1024),
        name="write_out",
    )(*halves)


def solution(mesh):
    placed = (
        P("sample", "gz", None, None),
        P("sample", "gz", None, None),
        P("gz", "sample", None),
        P("gz", "sample", None),
        P("gz", "sample", None),
        P("sample", "gz", None, None),
        P("sample"),
        P("gz", "sample", None),
        P("sample", "gz", None, None),
        P("sample", "gz", None, None),
    )
    return jax.shard_map(
        on_device,
        mesh=mesh,
        in_specs=placed,
        out_specs=(P("sample", "gz", None, None), P("gz", "sample", None), P("gz", "sample", None)),
        check_vma=False,
    )
```

```python
import jax
import jax.numpy as jnp
from jax import lax
from jax.experimental import pallas as pl
from jax.experimental.pallas import tpu as pltpu
from jax.sharding import PartitionSpec as P

STEPS = 8
PAIRS = 4
WANTED = [("sy", i, j) for i in range(PAIRS) for j in range(i, PAIRS)]
WANTED += [("yy", i, j) for i in range(PAIRS) for j in range(i, PAIRS)]
ROWS = 16
PAD = 8
LANES = 128
MESH = pl.DeviceIdType.MESH


def kernel(
    now, before, lame, shear, density, source, wave, prior, steps, changes,
    final, grad, s_vec, y_vec, total,
    wavelet, field, halo, first_coef, second_coef, force, spare, products, row, rows,
    send_sem, recv_sem, load_sem, hello_sem, sum_send, sum_recv,
):
    me = lax.axis_index("gz")
    count = lax.axis_size("gz")
    nx = first_coef.shape[2]
    chunks = nx // ROWS
    padded = nx + 2 * PAD
    zero = jnp.zeros((8, LANES), jnp.float32)
    lane = lax.broadcasted_iota(jnp.int32, (8, LANES), 1)
    row_lane = lax.broadcasted_iota(jnp.int32, (1, LANES), 1)
    at_start = lane == 0
    at_end = lane == LANES - 1
    exists = (me > 0, me < count - 1)
    beside = (jnp.maximum(me - 1, 0), jnp.minimum(me + 1, count - 1))

    inner = pl.ds(PAD, nx)
    loads = []

    def load(src, dst_of):
        for h in range(2):
            copy = pltpu.make_async_copy(
                src.at[..., pl.ds(h * LANES, LANES)], dst_of(h), load_sem.at[len(loads)]
            )
            copy.start()
            loads.append(copy)

    barrier = pltpu.get_barrier_semaphore()
    for d in range(2):

        @pl.when(exists[d])
        def _():
            pl.semaphore_signal(barrier, inc=1, device_id={"gz": beside[d]}, device_id_type=MESH)

    load(now, lambda h: field.at[0, :, :, h, inner, :])

    for par in range(2):
        for c in range(3):
            for d in range(2):
                for h in range(2):
                    for edge in (0, padded - PAD):
                        field[par, c, d, h, edge : edge + 8, :] = zero
                        halo[par, d, c, h, edge : edge + 8, :] = zero
    for d in range(2):

        @pl.when(jnp.logical_not(exists[d]))
        def _():
            def clear(i, carry):
                at = pl.ds(pl.multiple_of(i * 8, 8), 8)
                for par in range(2):
                    for c in range(3):
                        for h in range(2):
                            halo[par, d, c, h, at, :] = zero
                return carry

            lax.fori_loop(0, padded // 8, clear, 0)

    for copy in loads:
        copy.wait()
    wave_copy = pltpu.make_async_copy(wave, wavelet, load_sem.at[18])
    wave_copy.start()
    load(lame, lambda h: first_coef.at[:, h])
    load(shear, lambda h: second_coef.at[:, h])
    load(density, lambda h: spare.at[:, h])
    load(source, lambda h: force.at[:, :, h])
    load(prior, lambda h: grad.at[:, h])
    load(before, lambda h: field.at[1, :, :, h, inner, :])
    pl.semaphore_wait(barrier, jnp.where(me > 0, 1, 0) + jnp.where(me < count - 1, 1, 0))

    def outgoing(par, d, j):
        at = pl.ds(pl.multiple_of(PAD + j * ROWS, 8), ROWS)
        return pltpu.make_async_remote_copy(
            src_ref=field.at[par, :, d, :, at, :],
            dst_ref=halo.at[par, 1 - d, :, :, at, :],
            send_sem=send_sem.at[par, d, j],
            recv_sem=recv_sem.at[par, 1 - d, j],
            device_id={"gz": beside[d]},
            device_id_type=MESH,
        )

    def incoming(par, d, j):
        at = pl.ds(pl.multiple_of(PAD + j * ROWS, 8), ROWS)
        return pltpu.make_async_remote_copy(
            src_ref=field.at[par, :, d, :, at, :],
            dst_ref=halo.at[par, d, :, :, at, :],
            send_sem=send_sem.at[par, d, j],
            recv_sem=recv_sem.at[par, d, j],
            device_id={"gz": beside[d]},
            device_id_type=MESH,
        )

    def send(par, j):
        for d in range(2):
            pl.when(exists[d])(lambda d=d: outgoing(par, d, j).start())

    def wait_sent(par, j):
        for d in range(2):
            pl.when(exists[d])(lambda d=d: outgoing(par, d, j).wait_send())

    def wait_halo(par, j):
        for d in range(2):
            pl.when(exists[d])(lambda d=d: incoming(par, d, j).wait_recv())

    rounds = []
    while 4 << len(rounds) < count:
        rounds.append(4 << len(rounds))

    def far(r, d):
        return me + rounds[r] if d else me - rounds[r]

    def within(r, d):
        return far(r, d) < count if d else far(r, d) >= 0

    def tell_far(r):
        for d in range(2):

            @pl.when(within(r, d))
            def _():
                pl.semaphore_signal(
                    hello_sem.at[r, 1 - d], inc=1, device_id={"gz": far(r, d)}, device_id_type=MESH
                )

    def hear_far(r):
        for d in range(2):

            @pl.when(within(r, d))
            def _():
                pl.semaphore_wait(hello_sem.at[r, d], 1)

    def acquaint(n):
        for r in range(len(rounds) + 1):

            @pl.when(n == 2 + r)
            def _():
                if r > 0:
                    hear_far(r - 1)
                if r < len(rounds):
                    tell_far(r)

    def first_send(j, carry):
        send(0, j)
        return carry

    lax.fori_loop(0, chunks, first_send, 0)

    wave_copy.wait()
    for copy in loads[2:14]:
        copy.wait()
    load(steps, lambda h: s_vec.at[:, :, h])
    load(changes, lambda h: y_vec.at[:, :, h])

    def prepare(i, carry):
        at = pl.ds(pl.multiple_of(i * 8, 8), 8)
        for p in range(2):
            for h in range(2):
                mu = second_coef[p, h, at, :]
                coeff = 0.04 / spare[p, h, at, :]
                first_coef[p, h, at, :] = 0.25 * coeff * (first_coef[p, h, at, :] + mu)
                second_coef[p, h, at, :] = coeff * mu
                grad[p, h, at, :] = mu - grad[p, h, at, :]
                for c in range(3):
                    force[c, p, h, at, :] = coeff * force[c, p, h, at, :]
        return carry

    lax.fori_loop(0, nx // 8, prepare, 0)

    for w in range(len(WANTED)):
        products[w] = zero

    def gram(j):
        for w, (kind, a, b) in enumerate(WANTED):
            part = products[w]
            for i in range(ROWS // 8):
                at = pl.ds(pl.multiple_of(j * ROWS + i * 8, 8), 8)
                for p in range(2):
                    for h in range(2):
                        one = s_vec if kind == "sy" else y_vec
                        part = part + one[a, p, h, at, :] * y_vec[b, p, h, at, :]
            products[w] = part

    def lanes_of(x, first):
        n = x.shape[0]
        sums = jnp.sum(jnp.sum(x, axis=1), axis=1, keepdims=True)
        there = lax.broadcasted_iota(jnp.int32, (n, LANES), 1)
        wanted = lax.broadcasted_iota(jnp.int32, (n, LANES), 0) + first
        return jnp.sum(jnp.where(there == wanted, sums, 0.0), axis=0, keepdims=True)

    def along_y(v):
        back = [pltpu.roll(x, 1, 1) for x in v]
        ahead = [pltpu.roll(x, LANES - 1, 1) for x in v]
        plus = (jnp.where(at_end, ahead[1], ahead[0]), jnp.where(at_end, 0.0, ahead[1]))
        minus = (jnp.where(at_start, 0.0, back[0]), jnp.where(at_start, back[0], back[1]))
        return plus, minus

    def add(a, b):
        return (a[0] + b[0], a[1] + b[1])

    def sub(a, b):
        return (a[0] - b[0], a[1] - b[1])

    def block(cur, nxt, amplitude, base, out=None):
        at = pl.ds(base, 8)

        def rows_of(c, z, offset):
            from_row = pl.ds(base + PAD + offset, 8)
            if z in (-1, 2):
                return tuple(halo[cur, 0 if z < 0 else 1, c, h, from_row, :] for h in range(2))
            return tuple(field[cur, c, z, h, from_row, :] for h in range(2))

        u = {(c, z): rows_of(c, z, 0) for c in range(3) for z in (-1, 0, 1, 2)}
        up = {}
        down = {}
        for c in range(3):
            for z in (-1, 0, 1, 2) if c < 2 else (0, 1):
                up[c, z] = rows_of(c, z, 1)
                down[c, z] = rows_of(c, z, -1)
        dx = {key: sub(up[key], down[key]) for key in up}
        dy2 = {}
        sy = {}
        for z in (-1, 0, 1, 2):
            plus, minus = along_y(u[2, z])
            dy2[z] = sub(plus, minus)
            if z in (0, 1):
                sy[2, z] = add(plus, minus)
        mix0 = {z: add(dx[1, z], dy2[z]) for z in (-1, 0, 1, 2)}
        grads = []
        for z in range(2):
            for c in range(2):
                sy[c, z] = add(*along_y(u[c, z]))
            dz0 = sub(u[0, z + 1], u[0, z - 1])
            cross = [
                sub(mix0[z + 1], mix0[z - 1]),
                add(sub(dx[0, z + 1], dx[0, z - 1]), sub(*along_y(dx[2, z]))),
                sub(*along_y(add(dz0, dx[1, z]))),
            ]
            work = [None, None]
            for c in range(3):
                sz = add(u[c, z + 1], u[c, z - 1])
                sx = add(up[c, z], down[c, z])
                own = (sz, sx, sy[c, z])[c]
                for h in range(2):
                    centre = u[c, z][h]
                    twice = centre + centre
                    laplace = sz[h] + sx[h] + sy[c, z][h] - 6.0 * centre
                    div = 4.0 * (own[h] - twice) + cross[c][h]
                    new = (
                        twice
                        - field[nxt, c, z, h, pl.ds(base + PAD, 8), :]
                        + first_coef[z, h, at, :] * div
                        + second_coef[z, h, at, :] * laplace
                        + amplitude * force[c, z, h, at, :]
                    )
                    if out is None:
                        field[nxt, c, z, h, pl.ds(base + PAD, 8), :] = new
                    else:
                        out[c, z, h, at, :] = new
                    term = centre * laplace
                    work[h] = term if work[h] is None else work[h] + term
            for h in range(2):
                new = grad[z, h, at, :] + 0.02 * work[h]
                grad[z, h, at, :] = new
                grads.append((z, h, new))
        return grads

    def step(n, carry):
        cur = lax.rem(n, 2)
        nxt = 1 - cur
        amplitude = wavelet[n]
        wait_halo(cur, 0)
        acquaint(n)

        @pl.when(n == 1)
        def _():
            for copy in loads[14:]:
                copy.wait()

        @pl.when(n == 2)
        def _():
            row[...] = lanes_of(products[...], 2 * PAIRS)

        def chunk(j, inside):
            pl.when(j + 1 < chunks)(lambda: wait_halo(cur, j + 1))
            pl.when(n >= 1)(lambda: wait_sent(nxt, j))
            for b in range(ROWS // 8):
                block(cur, nxt, amplitude, pl.multiple_of(j * ROWS + b * 8, 8))
            send(nxt, j)
            pl.when(n == 1)(lambda: gram(j))
            return inside

        return lax.fori_loop(0, chunks, chunk, carry)

    lax.fori_loop(0, STEPS - 1, step, 0)

    cur, nxt = (STEPS - 1) % 2, STEPS % 2
    wait_halo(cur, 0)

    def last_chunk(j, sums):
        pl.when(j + 1 < chunks)(lambda: wait_halo(cur, j + 1))
        sums = list(sums)
        for b in range(ROWS // 8):
            base = pl.multiple_of(j * ROWS + b * 8, 8)
            for z, h, g in block(cur, nxt, wavelet[STEPS - 1], base, final):
                for k in range(PAIRS):
                    sums[k] = sums[k] + s_vec[k, z, h, pl.ds(base, 8), :] * g
                    sums[PAIRS + k] = sums[PAIRS + k] + y_vec[k, z, h, pl.ds(base, 8), :] * g
        return tuple(sums)

    sums = lax.fori_loop(0, chunks, last_chunk, (zero,) * (2 * PAIRS))

    rows[pl.ds(me, 1)] = (row[...] + lanes_of(jnp.stack(sums), 0))[None]

    for k in range(count - 1):
        pltpu.make_async_remote_copy(
            src_ref=rows.at[me],
            dst_ref=rows.at[me],
            send_sem=sum_send.at[0],
            recv_sem=sum_recv.at[0],
            device_id={"gz": k + jnp.where(me <= k, 1, 0)},
            device_id_type=MESH,
        ).start()

    def last_sent(j, carry):
        wait_sent(nxt, j)
        wait_sent(cur, j)
        return carry

    lax.fori_loop(0, chunks, last_sent, 0)

    others = rows.at[pl.ds(0, count - 1)]
    everyone = pltpu.make_async_remote_copy(
        src_ref=others,
        dst_ref=others,
        send_sem=sum_send.at[0],
        recv_sem=sum_recv.at[0],
        device_id={"gz": lax.rem(me + 1, count)},
        device_id_type=MESH,
    )
    everyone.wait_send()
    everyone.wait_recv()
    total[...] = jnp.sum(rows[...], axis=0)


def finish(
    final, grad, s_vec, y_vec, total, out_field, out_gradient, out_direction, result, sem
):
    copies = []

    def store(src, dst, h):
        copy = pltpu.make_async_copy(
            src, dst.at[..., pl.ds(h * LANES, LANES)], sem.at[len(copies)]
        )
        copy.start()
        copies.append(copy)

    for h in range(2):
        store(final.at[:, :, h], out_field, h)
        store(grad.at[:, h], out_gradient, h)

    nx = grad.shape[2]
    lane = lax.broadcasted_iota(jnp.int32, (1, LANES), 1)
    sums = total[...]

    def value(k):
        return jnp.sum(jnp.where(lane == k, sums, 0.0), axis=1, keepdims=True)

    sg = [value(k) for k in range(PAIRS)]
    yg = [value(PAIRS + k) for k in range(PAIRS)]
    pair = {}
    for w, (kind, a, b) in enumerate(WANTED):
        pair[kind, a, b] = value(2 * PAIRS + w)
        if kind == "yy":
            pair[kind, b, a] = pair[kind, a, b]
    rho = [1.0 / pair["sy", i, i] for i in range(PAIRS)]
    alphas = [None] * PAIRS
    for i in reversed(range(PAIRS)):
        dot = sg[i]
        for j in reversed(range(i + 1, PAIRS)):
            dot = dot - alphas[j] * pair["sy", i, j]
        alphas[i] = dot * rho[i]
    gamma = pair["sy", PAIRS - 1, PAIRS - 1] / pair["yy", PAIRS - 1, PAIRS - 1]
    extra = []
    for i in range(PAIRS):
        dot = yg[i]
        for j in range(PAIRS):
            dot = dot - alphas[j] * pair["yy", i, j]
        dot = gamma * dot
        for j in range(i):
            dot = dot + extra[j] * pair["sy", j, i]
        extra.append(alphas[i] - dot * rho[i])

    def wide(x):
        return jnp.broadcast_to(x, (8, LANES))

    of_g = wide(-gamma)
    of_y = [wide(gamma * alphas[i]) for i in range(PAIRS)]
    of_s = [wide(-extra[i]) for i in range(PAIRS)]
    for p in range(2):

        def combine(i, carry):
            at = pl.ds(pl.multiple_of(i * 8, 8), 8)
            for h in range(2):
                parts = [of_g * grad[p, h, at, :], of_s[0] * s_vec[0, p, h, at, :]]
                for k in range(PAIRS):
                    parts[0] = parts[0] + of_y[k] * y_vec[k, p, h, at, :]
                    if k > 0:
                        parts[1] = parts[1] + of_s[k] * s_vec[k, p, h, at, :]
                result[p, h, at, :] = parts[0] + parts[1]
            return carry

        lax.fori_loop(0, nx // 8, combine, 0, unroll=4)
        for h in range(2):
            store(result.at[p, h], out_direction.at[p], h)
    for copy in copies:
        copy.wait()


def on_device(*args):
    now = args[0]
    lame = args[2]
    nx = now.shape[2]
    count = lax.axis_size("gz")
    padded = nx + 2 * PAD
    chunks = nx // ROWS
    f32 = jnp.float32
    hbm = pl.BlockSpec(memory_space=pltpu.HBM)
    vmem = pl.BlockSpec(memory_space=pltpu.VMEM)
    in_specs = [hbm] * 10
    plane = (2, 2, nx, LANES)
    halves = pl.pallas_call(
        kernel,
        out_shape=(
            jax.ShapeDtypeStruct((3, *plane), f32),
            jax.ShapeDtypeStruct(plane, f32),
            jax.ShapeDtypeStruct((PAIRS, *plane), f32),
            jax.ShapeDtypeStruct((PAIRS, *plane), f32),
            jax.ShapeDtypeStruct((1, LANES), f32),
        ),
        in_specs=in_specs,
        out_specs=(vmem,) * 5,
        scratch_shapes=[
            pltpu.SMEM((STEPS,), f32),
            pltpu.VMEM((2, 3, 2, 2, padded, LANES), f32),
            pltpu.VMEM((2, 2, 3, 2, padded, LANES), f32),
            pltpu.VMEM(plane, f32),
            pltpu.VMEM(plane, f32),
            pltpu.VMEM((3, *plane), f32),
            pltpu.VMEM(plane, f32),
            pltpu.VMEM((len(WANTED), 8, LANES), f32),
            pltpu.VMEM((1, LANES), f32),
            pltpu.VMEM((count, 1, LANES), f32),
            pltpu.SemaphoreType.DMA((2, 2, chunks)),
            pltpu.SemaphoreType.DMA((2, 2, chunks)),
            pltpu.SemaphoreType.DMA((19,)),
            pltpu.SemaphoreType.REGULAR((3, 2)),
            pltpu.SemaphoreType.DMA((1,)),
            pltpu.SemaphoreType.DMA((1,)),
        ],
        compiler_params=pltpu.CompilerParams(
            collective_id=0, has_side_effects=True, vmem_limit_bytes=20 * 1024 * 1024
        ),
        name="leapfrog",
    )(*[pltpu.with_memory_space_constraint(x, pltpu.HBM) for x in args])
    return pl.pallas_call(
        finish,
        out_shape=(
            jax.ShapeDtypeStruct(now.shape, f32),
            jax.ShapeDtypeStruct(lame.shape, f32),
            jax.ShapeDtypeStruct(lame.shape, f32),
        ),
        in_specs=[vmem] * 5,
        out_specs=(hbm,) * 3,
        scratch_shapes=[pltpu.VMEM(plane, f32), pltpu.SemaphoreType.DMA((8,))],
        compiler_params=pltpu.CompilerParams(vmem_limit_bytes=8 * 1024 * 1024),
        name="finish",
    )(*halves)


def solution(mesh):
    placed = (
        P("sample", "gz", None, None),
        P("sample", "gz", None, None),
        P("gz", "sample", None),
        P("gz", "sample", None),
        P("gz", "sample", None),
        P("sample", "gz", None, None),
        P("sample"),
        P("gz", "sample", None),
        P("sample", "gz", None, None),
        P("sample", "gz", None, None),
    )
    return jax.shard_map(
        on_device,
        mesh=mesh,
        in_specs=placed,
        out_specs=(P("sample", "gz", None, None), P("gz", "sample", None), P("gz", "sample", None)),
        check_vma=False,
    )
```

```python
import jax
import jax.numpy as jnp
from jax import lax
from jax.experimental import pallas as pl
from jax.experimental.pallas import tpu as pltpu
from jax.sharding import PartitionSpec as P

STEPS = 8
PAIRS = 4
WANTED = [("sy", i, j) for i in range(PAIRS) for j in range(i, PAIRS)]
WANTED += [("yy", i, j) for i in range(PAIRS) for j in range(i, PAIRS)]
ROWS = 16
PAD = 8
LANES = 128
MESH = pl.DeviceIdType.MESH


def kernel(
    now, before, lame, shear, density, source, wave, prior, steps, changes,
    final, grad, s_vec, y_vec, total,
    wavelet, field, halo, bank, products, row, rows,
    link_send, link_recv, pair_send, pair_recv, load_sem, hello_sem, sum_send, sum_recv,
):
    me = lax.axis_index("gz")
    count = lax.axis_size("gz")
    nx = grad.shape[2]
    chunks = nx // ROWS
    half = chunks // 2
    padded = nx + 2 * PAD
    zero = jnp.zeros((8, LANES), jnp.float32)
    lane = lax.broadcasted_iota(jnp.int32, (8, LANES), 1)
    row_lane = lax.broadcasted_iota(jnp.int32, (1, LANES), 1)
    at_start = lane == 0
    at_end = lane == LANES - 1
    exists = (me > 0, me < count - 1)
    first_coef, second_coef, density_of, prior_of = (bank.at[k] for k in range(4))
    force = bank.at[pl.ds(4, 3)]

    core = lax.rem(me, 2)
    pair, link = 1 - core, core
    pair_peer = me + 1 - 2 * core
    linked = jnp.logical_and(me + 2 * core - 1 >= 0, me + 2 * core - 1 < count)
    link_peer = jnp.clip(me + 2 * core - 1, 0, count - 1)

    barrier = pltpu.get_barrier_semaphore()
    pl.semaphore_signal(barrier, inc=1, device_id={"gz": pair_peer}, device_id_type=MESH)

    @pl.when(linked)
    def _():
        pl.semaphore_signal(barrier, inc=1, device_id={"gz": link_peer}, device_id_type=MESH)

    inner = pl.ds(PAD, nx)

    def load(src, dst_of, group):
        for h in range(2):
            pltpu.make_async_copy(
                src.at[..., pl.ds(h * LANES, LANES)], dst_of(h), load_sem.at[group]
            ).start()

    def loaded(dst, group):
        pltpu.make_async_copy(dst, dst, load_sem.at[group]).wait()

    load(now, lambda h: field.at[0, :, :, h, inner, :], 0)

    for par in range(2):
        for c in range(3):
            for d in range(2):
                for h in range(2):
                    for edge in (0, padded - PAD):
                        field[par, c, d, h, edge : edge + 8, :] = zero
                        halo[par, d, c, h, edge : edge + 8, :] = zero
    for d in range(2):

        @pl.when(jnp.logical_not(exists[d]))
        def _():
            def clear(i, carry):
                at = pl.ds(pl.multiple_of(i * 8, 8), 8)
                for par in range(2):
                    for c in range(3):
                        for h in range(2):
                            halo[par, d, c, h, at, :] = zero
                return carry

            lax.fori_loop(0, padded // 8, clear, 0)

    pl.semaphore_wait(barrier, jnp.where(linked, 2, 1))

    def link_rows(j):
        return pl.multiple_of(j * ROWS, 8), ROWS

    def pair_rows(i):
        return i * half * ROWS, half * ROWS

    def over_link(par, start, size, sem):
        at = pl.ds(PAD + start, size)
        return pltpu.make_async_remote_copy(
            src_ref=field.at[par, :, link, :, at, :],
            dst_ref=halo.at[par, 1 - link, :, :, at, :],
            send_sem=link_send.at[par],
            recv_sem=link_recv.at[par, sem],
            device_id={"gz": link_peer},
            device_id_type=MESH,
        )

    def to_pair(par, start, size, sem):
        at = pl.ds(PAD + start, size)
        return pltpu.make_async_remote_copy(
            src_ref=field.at[par, :, pair, :, at, :],
            dst_ref=halo.at[par, 1 - pair, :, :, at, :],
            send_sem=pair_send.at[par],
            recv_sem=pair_recv.at[par, sem],
            device_id={"gz": pair_peer},
            device_id_type=MESH,
        )

    def from_argument(direction, start, size, h, send_sem, recv_sem, peer):
        pltpu.make_async_remote_copy(
            src_ref=now.at[:, direction, pl.ds(start, size), pl.ds(h * LANES, LANES)],
            dst_ref=halo.at[0, 1 - direction, :, h, pl.ds(PAD + start, size), :],
            send_sem=send_sem,
            recv_sem=recv_sem,
            device_id={"gz": peer},
            device_id_type=MESH,
        ).start()

    def first_send(j, carry):
        for h in range(2):
            from_argument(
                link, *link_rows(j), h, link_send.at[0], link_recv.at[0, j], link_peer
            )
        return carry

    @pl.when(linked)
    def _():
        lax.fori_loop(0, chunks, first_send, 0)

    for i in range(2):
        for h in range(2):
            from_argument(
                pair, *pair_rows(i), h, pair_send.at[0], pair_recv.at[0, i], pair_peer
            )
    wave_copy = pltpu.make_async_copy(wave, wavelet, load_sem.at[3])
    wave_copy.start()
    load(lame, lambda h: first_coef.at[:, h], 1)
    load(shear, lambda h: second_coef.at[:, h], 1)
    load(density, lambda h: density_of.at[:, h], 1)
    load(prior, lambda h: prior_of.at[:, h], 1)
    load(source, lambda h: force.at[:, :, h], 1)
    load(before, lambda h: field.at[1, :, :, h, inner, :], 2)

    def send_link(par, j):
        pl.when(linked)(lambda: over_link(par, *link_rows(j), j).start())

    def send_pair(par, i):
        to_pair(par, *pair_rows(i), i).start()

    def wait_sent(par):
        to_pair(par, 0, nx, 0).wait_send()
        pl.when(linked)(lambda: over_link(par, 0, nx, 0).wait_send())

    def wait_link(par, j):
        @pl.when(linked)
        def _():
            start, size = link_rows(j)
            at = pl.ds(PAD + start, size)
            pltpu.make_async_remote_copy(
                src_ref=field.at[par, :, link, :, at, :],
                dst_ref=halo.at[par, link, :, :, at, :],
                send_sem=link_send.at[par],
                recv_sem=link_recv.at[par, j],
                device_id={"gz": link_peer},
                device_id_type=MESH,
            ).wait_recv()

    def wait_pair(par, i):
        start, size = pair_rows(i)
        at = pl.ds(PAD + start, size)
        pltpu.make_async_remote_copy(
            src_ref=field.at[par, :, pair, :, at, :],
            dst_ref=halo.at[par, pair, :, :, at, :],
            send_sem=pair_send.at[par],
            recv_sem=pair_recv.at[par, i],
            device_id={"gz": pair_peer},
            device_id_type=MESH,
        ).wait_recv()

    rounds = []
    while 4 << len(rounds) < count:
        rounds.append(4 << len(rounds))

    def far(r, d):
        return me + rounds[r] if d else me - rounds[r]

    def within(r, d):
        return far(r, d) < count if d else far(r, d) >= 0

    def tell_far(r):
        for d in range(2):

            @pl.when(within(r, d))
            def _():
                pl.semaphore_signal(
                    hello_sem.at[r], inc=1, device_id={"gz": far(r, d)}, device_id_type=MESH
                )

    def hear_far(r):
        heard = jnp.where(within(r, 0), 1, 0) + jnp.where(within(r, 1), 1, 0)
        pl.when(heard > 0)(lambda: pl.semaphore_wait(hello_sem.at[r], heard))

    def acquaint(n):
        for r in range(len(rounds) + 1):

            @pl.when(n == 2 + r)
            def _():
                if r > 0:
                    hear_far(r - 1)
                if r < len(rounds):
                    tell_far(r)


    wave_copy.wait()
    loaded(bank, 1)
    loaded(field.at[0, :, :, :, inner, :], 0)
    loaded(field.at[1, :, :, :, inner, :], 2)
    load(steps, lambda h: s_vec.at[:, :, h], 4)
    load(changes, lambda h: y_vec.at[:, :, h], 5)

    def prepare(i, carry):
        at = pl.ds(pl.multiple_of(i * 8, 8), 8)
        for p in range(2):
            for h in range(2):
                mu = second_coef[p, h, at, :]
                coeff = 0.04 / density_of[p, h, at, :]
                first_coef[p, h, at, :] = 0.25 * coeff * (first_coef[p, h, at, :] + mu)
                second_coef[p, h, at, :] = coeff * mu
                grad[p, h, at, :] = mu - prior_of[p, h, at, :]
                for c in range(3):
                    force[c, p, h, at, :] = coeff * force[c, p, h, at, :]
        return carry

    lax.fori_loop(0, nx // 8, prepare, 0)

    for w in range(len(WANTED)):
        products[w] = zero

    def gram(j):
        for w, (kind, a, b) in enumerate(WANTED):
            part = products[w]
            for i in range(ROWS // 8):
                at = pl.ds(pl.multiple_of(j * ROWS + i * 8, 8), 8)
                for p in range(2):
                    for h in range(2):
                        one = s_vec if kind == "sy" else y_vec
                        part = part + one[a, p, h, at, :] * y_vec[b, p, h, at, :]
            products[w] = part

    def lanes_of(x, first):
        n = x.shape[0]
        sums = jnp.sum(jnp.sum(x, axis=1), axis=1, keepdims=True)
        there = lax.broadcasted_iota(jnp.int32, (n, LANES), 1)
        wanted = lax.broadcasted_iota(jnp.int32, (n, LANES), 0) + first
        return jnp.sum(jnp.where(there == wanted, sums, 0.0), axis=0, keepdims=True)

    def along_y(v):
        back = [pltpu.roll(x, 1, 1) for x in v]
        ahead = [pltpu.roll(x, LANES - 1, 1) for x in v]
        plus = (jnp.where(at_end, ahead[1], ahead[0]), jnp.where(at_end, 0.0, ahead[1]))
        minus = (jnp.where(at_start, 0.0, back[0]), jnp.where(at_start, back[0], back[1]))
        return plus, minus

    def add(a, b):
        return (a[0] + b[0], a[1] + b[1])

    def sub(a, b):
        return (a[0] - b[0], a[1] - b[1])

    def block(cur, nxt, amplitude, base, out=None):
        at = pl.ds(base, 8)

        def rows_of(c, z, offset):
            from_row = pl.ds(base + PAD + offset, 8)
            if z in (-1, 2):
                return tuple(halo[cur, 0 if z < 0 else 1, c, h, from_row, :] for h in range(2))
            return tuple(field[cur, c, z, h, from_row, :] for h in range(2))

        u = {(c, z): rows_of(c, z, 0) for c in range(3) for z in (-1, 0, 1, 2)}
        up = {}
        down = {}
        for c in range(3):
            for z in (-1, 0, 1, 2) if c < 2 else (0, 1):
                up[c, z] = rows_of(c, z, 1)
                down[c, z] = rows_of(c, z, -1)
        dx = {key: sub(up[key], down[key]) for key in up}
        dy2 = {}
        sy = {}
        for z in (-1, 0, 1, 2):
            plus, minus = along_y(u[2, z])
            dy2[z] = sub(plus, minus)
            if z in (0, 1):
                sy[2, z] = add(plus, minus)
        mix0 = {z: add(dx[1, z], dy2[z]) for z in (-1, 0, 1, 2)}
        grads = []
        for z in range(2):
            for c in range(2):
                sy[c, z] = add(*along_y(u[c, z]))
            dz0 = sub(u[0, z + 1], u[0, z - 1])
            cross = [
                sub(mix0[z + 1], mix0[z - 1]),
                add(sub(dx[0, z + 1], dx[0, z - 1]), sub(*along_y(dx[2, z]))),
                sub(*along_y(add(dz0, dx[1, z]))),
            ]
            work = [None, None]
            for c in range(3):
                sz = add(u[c, z + 1], u[c, z - 1])
                sx = add(up[c, z], down[c, z])
                own = (sz, sx, sy[c, z])[c]
                for h in range(2):
                    centre = u[c, z][h]
                    twice = centre + centre
                    laplace = sz[h] + sx[h] + sy[c, z][h] - 6.0 * centre
                    div = 4.0 * (own[h] - twice) + cross[c][h]
                    new = (
                        twice
                        - field[nxt, c, z, h, pl.ds(base + PAD, 8), :]
                        + first_coef[z, h, at, :] * div
                        + second_coef[z, h, at, :] * laplace
                        + amplitude * force[c, z, h, at, :]
                    )
                    if out is None:
                        field[nxt, c, z, h, pl.ds(base + PAD, 8), :] = new
                    else:
                        out[c, z, h, at, :] = new
                    term = centre * laplace
                    work[h] = term if work[h] is None else work[h] + term
            for h in range(2):
                new = grad[z, h, at, :] + 0.02 * work[h]
                grad[z, h, at, :] = new
                grads.append((z, h, new))
        return grads

    def step(n, carry):
        cur = lax.rem(n, 2)
        nxt = 1 - cur
        amplitude = wavelet[n]
        wait_link(cur, 0)
        wait_pair(cur, 0)
        pl.when(n >= 1)(lambda: wait_sent(nxt))
        acquaint(n)

        @pl.when(n == 1)
        def _():
            loaded(s_vec, 4)
            loaded(y_vec, 5)

        @pl.when(n == 2)
        def _():
            row[...] = lanes_of(products[...], 2 * PAIRS)

        def chunk(j, inside):
            pl.when(j + 1 < chunks)(lambda: wait_link(cur, j + 1))
            pl.when(j == half - 1)(lambda: wait_pair(cur, 1))
            for b in range(ROWS // 8):
                block(cur, nxt, amplitude, pl.multiple_of(j * ROWS + b * 8, 8))
            send_link(nxt, j)
            pl.when(j == half - 1)(lambda: send_pair(nxt, 0))
            pl.when(n == 1)(lambda: gram(j))
            return inside

        lax.fori_loop(0, chunks, chunk, 0)
        send_pair(nxt, 1)
        return carry

    lax.fori_loop(0, STEPS - 1, step, 0)

    cur, nxt = (STEPS - 1) % 2, STEPS % 2
    wait_link(cur, 0)
    wait_pair(cur, 0)

    def last_chunk(j, sums):
        pl.when(j + 1 < chunks)(lambda: wait_link(cur, j + 1))
        pl.when(j == half - 1)(lambda: wait_pair(cur, 1))
        sums = list(sums)
        for b in range(ROWS // 8):
            base = pl.multiple_of(j * ROWS + b * 8, 8)
            for z, h, g in block(cur, nxt, wavelet[STEPS - 1], base, final):
                for k in range(PAIRS):
                    sums[k] = sums[k] + s_vec[k, z, h, pl.ds(base, 8), :] * g
                    sums[PAIRS + k] = sums[PAIRS + k] + y_vec[k, z, h, pl.ds(base, 8), :] * g
        return tuple(sums)

    sums = lax.fori_loop(0, chunks, last_chunk, (zero,) * (2 * PAIRS))

    rows[pl.ds(me, 1)] = (row[...] + lanes_of(jnp.stack(sums), 0))[None]

    for k in range(count - 1):
        pltpu.make_async_remote_copy(
            src_ref=rows.at[me],
            dst_ref=rows.at[me],
            send_sem=sum_send.at[0],
            recv_sem=sum_recv.at[0],
            device_id={"gz": k + jnp.where(me <= k, 1, 0)},
            device_id_type=MESH,
        ).start()

    wait_sent(nxt)
    wait_sent(cur)

    others = rows.at[pl.ds(0, count - 1)]
    everyone = pltpu.make_async_remote_copy(
        src_ref=others,
        dst_ref=others,
        send_sem=sum_send.at[0],
        recv_sem=sum_recv.at[0],
        device_id={"gz": lax.rem(me + 1, count)},
        device_id_type=MESH,
    )
    everyone.wait_send()
    everyone.wait_recv()
    total[...] = jnp.sum(rows[...], axis=0)


def finish(
    final, grad, s_vec, y_vec, total, out_field, out_gradient, out_direction, result, sem
):
    def store(src, dst, h, group):
        pltpu.make_async_copy(src, dst.at[..., pl.ds(h * LANES, LANES)], sem.at[group]).start()

    for h in range(2):
        store(final.at[:, :, h], out_field, h, 0)
        store(grad.at[:, h], out_gradient, h, 1)

    nx = grad.shape[2]
    lane = lax.broadcasted_iota(jnp.int32, (1, LANES), 1)
    sums = total[...]

    def value(k):
        return jnp.sum(jnp.where(lane == k, sums, 0.0), axis=1, keepdims=True)

    sg = [value(k) for k in range(PAIRS)]
    yg = [value(PAIRS + k) for k in range(PAIRS)]
    pair = {}
    for w, (kind, a, b) in enumerate(WANTED):
        pair[kind, a, b] = value(2 * PAIRS + w)
        if kind == "yy":
            pair[kind, b, a] = pair[kind, a, b]
    rho = [1.0 / pair["sy", i, i] for i in range(PAIRS)]
    alphas = [None] * PAIRS
    for i in reversed(range(PAIRS)):
        dot = sg[i]
        for j in reversed(range(i + 1, PAIRS)):
            dot = dot - alphas[j] * pair["sy", i, j]
        alphas[i] = dot * rho[i]
    gamma = pair["sy", PAIRS - 1, PAIRS - 1] / pair["yy", PAIRS - 1, PAIRS - 1]
    extra = []
    for i in range(PAIRS):
        dot = yg[i]
        for j in range(PAIRS):
            dot = dot - alphas[j] * pair["yy", i, j]
        dot = gamma * dot
        for j in range(i):
            dot = dot + extra[j] * pair["sy", j, i]
        extra.append(alphas[i] - dot * rho[i])

    def wide(x):
        return jnp.broadcast_to(x, (8, LANES))

    of_g = wide(-gamma)
    of_y = [wide(gamma * alphas[i]) for i in range(PAIRS)]
    of_s = [wide(-extra[i]) for i in range(PAIRS)]
    for p in range(2):

        def combine(i, carry):
            at = pl.ds(pl.multiple_of(i * 8, 8), 8)
            for h in range(2):
                parts = [of_g * grad[p, h, at, :], of_s[0] * s_vec[0, p, h, at, :]]
                for k in range(PAIRS):
                    parts[0] = parts[0] + of_y[k] * y_vec[k, p, h, at, :]
                    if k > 0:
                        parts[1] = parts[1] + of_s[k] * s_vec[k, p, h, at, :]
                result[p, h, at, :] = parts[0] + parts[1]
            return carry

        lax.fori_loop(0, nx // 8, combine, 0, unroll=4)
        for h in range(2):
            store(result.at[p, h], out_direction.at[p], h, 2)
    for group, out in enumerate((out_field, out_gradient, out_direction)):
        pltpu.make_async_copy(out, out, sem.at[group]).wait()


def on_device(*args):
    now = args[0]
    lame = args[2]
    nx = now.shape[2]
    count = lax.axis_size("gz")
    padded = nx + 2 * PAD
    chunks = nx // ROWS
    f32 = jnp.float32
    hbm = pl.BlockSpec(memory_space=pltpu.HBM)
    vmem = pl.BlockSpec(memory_space=pltpu.VMEM)
    in_specs = [hbm] * 10
    plane = (2, 2, nx, LANES)
    halves = pl.pallas_call(
        kernel,
        out_shape=(
            jax.ShapeDtypeStruct((3, *plane), f32),
            jax.ShapeDtypeStruct(plane, f32),
            jax.ShapeDtypeStruct((PAIRS, *plane), f32),
            jax.ShapeDtypeStruct((PAIRS, *plane), f32),
            jax.ShapeDtypeStruct((1, LANES), f32),
        ),
        in_specs=in_specs,
        out_specs=(vmem,) * 5,
        scratch_shapes=[
            pltpu.SMEM((STEPS,), f32),
            pltpu.VMEM((2, 3, 2, 2, padded, LANES), f32),
            pltpu.VMEM((2, 2, 3, 2, padded, LANES), f32),
            pltpu.VMEM((7, *plane), f32),
            pltpu.VMEM((len(WANTED), 8, LANES), f32),
            pltpu.VMEM((1, LANES), f32),
            pltpu.VMEM((count, 1, LANES), f32),
            pltpu.SemaphoreType.DMA((2,)),
            pltpu.SemaphoreType.DMA((2, chunks)),
            pltpu.SemaphoreType.DMA((2,)),
            pltpu.SemaphoreType.DMA((2, 2)),
            pltpu.SemaphoreType.DMA((6,)),
            pltpu.SemaphoreType.REGULAR((3,)),
            pltpu.SemaphoreType.DMA((1,)),
            pltpu.SemaphoreType.DMA((1,)),
        ],
        compiler_params=pltpu.CompilerParams(
            collective_id=0, has_side_effects=True, vmem_limit_bytes=20 * 1024 * 1024
        ),
        name="leapfrog",
    )(*[pltpu.with_memory_space_constraint(x, pltpu.HBM) for x in args])
    return pl.pallas_call(
        finish,
        out_shape=(
            jax.ShapeDtypeStruct(now.shape, f32),
            jax.ShapeDtypeStruct(lame.shape, f32),
            jax.ShapeDtypeStruct(lame.shape, f32),
        ),
        in_specs=[vmem] * 5,
        out_specs=(hbm,) * 3,
        scratch_shapes=[pltpu.VMEM(plane, f32), pltpu.SemaphoreType.DMA((3,))],
        compiler_params=pltpu.CompilerParams(vmem_limit_bytes=8 * 1024 * 1024),
        name="finish",
    )(*halves)


def solution(mesh):
    placed = (
        P("sample", "gz", None, None),
        P("sample", "gz", None, None),
        P("gz", "sample", None),
        P("gz", "sample", None),
        P("gz", "sample", None),
        P("sample", "gz", None, None),
        P("sample"),
        P("gz", "sample", None),
        P("sample", "gz", None, None),
        P("sample", "gz", None, None),
    )
    return jax.shard_map(
        on_device,
        mesh=mesh,
        in_specs=placed,
        out_specs=(P("sample", "gz", None, None), P("gz", "sample", None), P("gz", "sample", None)),
        check_vma=False,
    )
```

```python
import jax
import jax.numpy as jnp
from jax import lax
from jax.experimental import pallas as pl
from jax.experimental.pallas import tpu as pltpu
from jax.sharding import PartitionSpec as P

STEPS = 8
PAIRS = 4
WANTED = [("sy", i, j) for i in range(PAIRS) for j in range(i, PAIRS)]
WANTED += [("yy", i, j) for i in range(PAIRS) for j in range(i, PAIRS)]
ROWS = 24
REST = 16
PAD = 8
LANES = 128
MESH = pl.DeviceIdType.MESH


def kernel(
    now, before, lame, shear, density, source, wave, prior, steps, changes,
    final, grad, s_vec, y_vec, total,
    wavelet, field, halo, bank, products, row, rows,
    link_send, link_recv, pair_send, pair_recv, load_sem, hello_sem, sum_send, sum_recv,
):
    me = lax.axis_index("gz")
    count = lax.axis_size("gz")
    nx = grad.shape[2]
    last = (nx - REST) // ROWS
    split = (last + 1) // 2
    padded = nx + 2 * PAD
    zero = jnp.zeros((8, LANES), jnp.float32)
    lane = lax.broadcasted_iota(jnp.int32, (8, LANES), 1)
    row_lane = lax.broadcasted_iota(jnp.int32, (1, LANES), 1)
    at_start = lane == 0
    at_end = lane == LANES - 1
    exists = (me > 0, me < count - 1)
    first_coef, second_coef, density_of, prior_of = (bank.at[k] for k in range(4))
    force = bank.at[pl.ds(4, 3)]

    core = lax.rem(me, 2)
    pair, link = 1 - core, core
    pair_peer = me + 1 - 2 * core
    linked = jnp.logical_and(me + 2 * core - 1 >= 0, me + 2 * core - 1 < count)
    link_peer = jnp.clip(me + 2 * core - 1, 0, count - 1)

    barrier = pltpu.get_barrier_semaphore()
    pl.semaphore_signal(barrier, inc=1, device_id={"gz": pair_peer}, device_id_type=MESH)

    @pl.when(linked)
    def _():
        pl.semaphore_signal(barrier, inc=1, device_id={"gz": link_peer}, device_id_type=MESH)

    inner = pl.ds(PAD, nx)

    def load(src, dst_of, group):
        for h in range(2):
            pltpu.make_async_copy(
                src.at[..., pl.ds(h * LANES, LANES)], dst_of(h), load_sem.at[group]
            ).start()

    def loaded(dst, group):
        pltpu.make_async_copy(dst, dst, load_sem.at[group]).wait()

    load(now, lambda h: field.at[0, :, :, h, inner, :], 0)

    for par in range(2):
        for c in range(3):
            for d in range(2):
                for h in range(2):
                    for edge in (0, padded - PAD):
                        field[par, c, d, h, edge : edge + 8, :] = zero
                        halo[par, d, c, h, edge : edge + 8, :] = zero
    for d in range(2):

        @pl.when(jnp.logical_not(exists[d]))
        def _():
            def clear(i, carry):
                at = pl.ds(pl.multiple_of(i * 8, 8), 8)
                for par in range(2):
                    for c in range(3):
                        for h in range(2):
                            halo[par, d, c, h, at, :] = zero
                return carry

            lax.fori_loop(0, padded // 8, clear, 0)

    pl.semaphore_wait(barrier, jnp.where(linked, 2, 1))

    def link_rows(j):
        if isinstance(j, int):
            return j * ROWS, REST if j == last else ROWS
        return pl.multiple_of(j * ROWS, 8), ROWS

    def pair_rows(i):
        return (split * ROWS, nx - split * ROWS) if i else (0, split * ROWS)

    def over_link(par, start, size, sem):
        at = pl.ds(PAD + start, size)
        return pltpu.make_async_remote_copy(
            src_ref=field.at[par, :, link, :, at, :],
            dst_ref=halo.at[par, 1 - link, :, :, at, :],
            send_sem=link_send.at[par],
            recv_sem=link_recv.at[par, sem],
            device_id={"gz": link_peer},
            device_id_type=MESH,
        )

    def to_pair(par, start, size, sem):
        at = pl.ds(PAD + start, size)
        return pltpu.make_async_remote_copy(
            src_ref=field.at[par, :, pair, :, at, :],
            dst_ref=halo.at[par, 1 - pair, :, :, at, :],
            send_sem=pair_send.at[par],
            recv_sem=pair_recv.at[par, sem],
            device_id={"gz": pair_peer},
            device_id_type=MESH,
        )

    def from_argument(direction, start, size, h, send_sem, recv_sem, peer):
        pltpu.make_async_remote_copy(
            src_ref=now.at[:, direction, pl.ds(start, size), pl.ds(h * LANES, LANES)],
            dst_ref=halo.at[0, 1 - direction, :, h, pl.ds(PAD + start, size), :],
            send_sem=send_sem,
            recv_sem=recv_sem,
            device_id={"gz": peer},
            device_id_type=MESH,
        ).start()

    def first_send(j, carry):
        for h in range(2):
            from_argument(
                link, *link_rows(j), h, link_send.at[0], link_recv.at[0, j], link_peer
            )
        return carry

    @pl.when(linked)
    def _():
        lax.fori_loop(0, last, first_send, 0)
        first_send(last, 0)

    for i in range(2):
        for h in range(2):
            from_argument(
                pair, *pair_rows(i), h, pair_send.at[0], pair_recv.at[0, i], pair_peer
            )
    wave_copy = pltpu.make_async_copy(wave, wavelet, load_sem.at[3])
    wave_copy.start()
    load(lame, lambda h: first_coef.at[:, h], 1)
    load(shear, lambda h: second_coef.at[:, h], 1)
    load(density, lambda h: density_of.at[:, h], 1)
    load(prior, lambda h: prior_of.at[:, h], 1)
    load(source, lambda h: force.at[:, :, h], 1)
    load(before, lambda h: field.at[1, :, :, h, inner, :], 2)

    def send_link(par, j):
        pl.when(linked)(lambda: over_link(par, *link_rows(j), j).start())

    def send_pair(par, i):
        to_pair(par, *pair_rows(i), i).start()

    def wait_sent(par):
        to_pair(par, 0, nx, 0).wait_send()
        pl.when(linked)(lambda: over_link(par, 0, nx, 0).wait_send())

    def wait_link(par, j):
        @pl.when(linked)
        def _():
            start, size = link_rows(j)
            at = pl.ds(PAD + start, size)
            pltpu.make_async_remote_copy(
                src_ref=field.at[par, :, link, :, at, :],
                dst_ref=halo.at[par, link, :, :, at, :],
                send_sem=link_send.at[par],
                recv_sem=link_recv.at[par, j],
                device_id={"gz": link_peer},
                device_id_type=MESH,
            ).wait_recv()

    def wait_pair(par, i):
        start, size = pair_rows(i)
        at = pl.ds(PAD + start, size)
        pltpu.make_async_remote_copy(
            src_ref=field.at[par, :, pair, :, at, :],
            dst_ref=halo.at[par, pair, :, :, at, :],
            send_sem=pair_send.at[par],
            recv_sem=pair_recv.at[par, i],
            device_id={"gz": pair_peer},
            device_id_type=MESH,
        ).wait_recv()

    rounds = []
    while 4 << len(rounds) < count:
        rounds.append(4 << len(rounds))

    def far(r, d):
        return me + rounds[r] if d else me - rounds[r]

    def within(r, d):
        return far(r, d) < count if d else far(r, d) >= 0

    def tell_far(r):
        for d in range(2):

            @pl.when(within(r, d))
            def _():
                pl.semaphore_signal(
                    hello_sem.at[r], inc=1, device_id={"gz": far(r, d)}, device_id_type=MESH
                )

    def hear_far(r):
        heard = jnp.where(within(r, 0), 1, 0) + jnp.where(within(r, 1), 1, 0)
        pl.when(heard > 0)(lambda: pl.semaphore_wait(hello_sem.at[r], heard))

    def acquaint(n):
        for r in range(len(rounds) + 1):

            @pl.when(n == 3 + r)
            def _():
                if r > 0:
                    hear_far(r - 1)
                if r < len(rounds):
                    tell_far(r)


    wave_copy.wait()
    loaded(bank, 1)
    loaded(field.at[0, :, :, :, inner, :], 0)
    loaded(field.at[1, :, :, :, inner, :], 2)
    load(steps, lambda h: s_vec.at[:, :, h], 4)
    load(changes, lambda h: y_vec.at[:, :, h], 5)

    def prepare(i, carry):
        at = pl.ds(pl.multiple_of(i * 8, 8), 8)
        for p in range(2):
            for h in range(2):
                mu = second_coef[p, h, at, :]
                coeff = 0.04 / density_of[p, h, at, :]
                first_coef[p, h, at, :] = 0.25 * coeff * (first_coef[p, h, at, :] + mu)
                second_coef[p, h, at, :] = coeff * mu
                grad[p, h, at, :] = mu - prior_of[p, h, at, :]
                for c in range(3):
                    force[c, p, h, at, :] = coeff * force[c, p, h, at, :]
        return carry

    lax.fori_loop(0, nx // 8, prepare, 0)

    for w in range(len(WANTED)):
        products[w] = zero

    def gram(bases):
        for w, (kind, a, b) in enumerate(WANTED):
            part = products[w]
            for base in bases:
                at = pl.ds(base, 8)
                for p in range(2):
                    for h in range(2):
                        one = s_vec if kind == "sy" else y_vec
                        part = part + one[a, p, h, at, :] * y_vec[b, p, h, at, :]
            products[w] = part

    def lanes_of(x, first):
        n = x.shape[0]
        sums = jnp.sum(jnp.sum(x, axis=1), axis=1, keepdims=True)
        there = lax.broadcasted_iota(jnp.int32, (n, LANES), 1)
        wanted = lax.broadcasted_iota(jnp.int32, (n, LANES), 0) + first
        return jnp.sum(jnp.where(there == wanted, sums, 0.0), axis=0, keepdims=True)

    def along_y(v):
        back = [pltpu.roll(x, 1, 1) for x in v]
        ahead = [pltpu.roll(x, LANES - 1, 1) for x in v]
        plus = (jnp.where(at_end, ahead[1], ahead[0]), jnp.where(at_end, 0.0, ahead[1]))
        minus = (jnp.where(at_start, 0.0, back[0]), jnp.where(at_start, back[0], back[1]))
        return plus, minus

    def add(a, b):
        return (a[0] + b[0], a[1] + b[1])

    def sub(a, b):
        return (a[0] - b[0], a[1] - b[1])

    def block(cur, nxt, amplitude, base, out=None):
        at = pl.ds(base, 8)

        def rows_of(c, z, offset):
            from_row = pl.ds(base + PAD + offset, 8)
            if z in (-1, 2):
                return tuple(halo[cur, 0 if z < 0 else 1, c, h, from_row, :] for h in range(2))
            return tuple(field[cur, c, z, h, from_row, :] for h in range(2))

        u = {(c, z): rows_of(c, z, 0) for c in range(3) for z in (-1, 0, 1, 2)}
        up = {}
        down = {}
        for c in range(3):
            for z in (-1, 0, 1, 2) if c < 2 else (0, 1):
                up[c, z] = rows_of(c, z, 1)
                down[c, z] = rows_of(c, z, -1)
        dx = {key: sub(up[key], down[key]) for key in up}
        dy2 = {}
        sy = {}
        for z in (-1, 0, 1, 2):
            plus, minus = along_y(u[2, z])
            dy2[z] = sub(plus, minus)
            if z in (0, 1):
                sy[2, z] = add(plus, minus)
        mix0 = {z: add(dx[1, z], dy2[z]) for z in (-1, 0, 1, 2)}
        grads = []
        for z in range(2):
            for c in range(2):
                sy[c, z] = add(*along_y(u[c, z]))
            dz0 = sub(u[0, z + 1], u[0, z - 1])
            cross = [
                sub(mix0[z + 1], mix0[z - 1]),
                add(sub(dx[0, z + 1], dx[0, z - 1]), sub(*along_y(dx[2, z]))),
                sub(*along_y(add(dz0, dx[1, z]))),
            ]
            work = [None, None]
            for c in range(3):
                sz = add(u[c, z + 1], u[c, z - 1])
                sx = add(up[c, z], down[c, z])
                own = (sz, sx, sy[c, z])[c]
                for h in range(2):
                    centre = u[c, z][h]
                    twice = centre + centre
                    laplace = sz[h] + sx[h] + sy[c, z][h] - 6.0 * centre
                    div = 4.0 * (own[h] - twice) + cross[c][h]
                    new = (
                        twice
                        - field[nxt, c, z, h, pl.ds(base + PAD, 8), :]
                        + first_coef[z, h, at, :] * div
                        + second_coef[z, h, at, :] * laplace
                        + amplitude * force[c, z, h, at, :]
                    )
                    if out is None:
                        field[nxt, c, z, h, pl.ds(base + PAD, 8), :] = new
                    else:
                        out[c, z, h, at, :] = new
                    term = centre * laplace
                    work[h] = term if work[h] is None else work[h] + term
            for h in range(2):
                new = grad[z, h, at, :] + 0.02 * work[h]
                grad[z, h, at, :] = new
                grads.append((z, h, new))
        return grads

    def sweep(cur, nxt, amplitude, out, after, ending, carry):
        def at_split(j, act):
            if isinstance(j, int):
                if j == split:
                    act()
            else:
                pl.when(j == split)(act)

        def part(j, bases, carry):
            wait_link(cur, j)
            at_split(j, lambda: wait_pair(cur, 1))
            for i, base in enumerate(bases):
                carry = after(base, block(cur, nxt, amplitude, base, out), carry)
                if i == 0 and out is None and not (isinstance(j, int) and j == 0):
                    send_link(nxt, j - 1)
                    at_split(j, lambda: send_pair(nxt, 0))
            ending(bases)
            return carry

        def later(j, carry):
            return part(j, [pl.multiple_of(j * ROWS + k, 8) for k in (-8, 0, 8)], carry)

        wait_pair(cur, 0)
        carry = part(0, [0, 8], carry)
        carry = lax.fori_loop(1, last, later, carry)
        carry = part(last, [last * ROWS + k for k in (-8, 0, 8)], carry)
        if out is None:
            send_link(nxt, last)
            send_pair(nxt, 1)
        return carry

    def step(n, carry):
        cur = lax.rem(n, 2)
        nxt = 1 - cur
        pl.when(n >= 1)(lambda: wait_sent(nxt))
        acquaint(n)

        @pl.when(n == 1)
        def _():
            loaded(s_vec, 4)
            loaded(y_vec, 5)

        @pl.when(n == 2)
        def _():
            row[...] = lanes_of(products[...], 2 * PAIRS)

        return sweep(
            cur,
            nxt,
            wavelet[n],
            None,
            lambda base, grads, carry: carry,
            lambda bases: pl.when(n == 1)(lambda: gram(bases)),
            carry,
        )

    lax.fori_loop(0, STEPS - 1, step, 0)

    cur, nxt = (STEPS - 1) % 2, STEPS % 2

    def multiply(base, grads, sums):
        sums = list(sums)
        for z, h, g in grads:
            for k in range(PAIRS):
                sums[k] = sums[k] + s_vec[k, z, h, pl.ds(base, 8), :] * g
                sums[PAIRS + k] = sums[PAIRS + k] + y_vec[k, z, h, pl.ds(base, 8), :] * g
        return tuple(sums)

    sums = sweep(
        cur,
        nxt,
        wavelet[STEPS - 1],
        final,
        multiply,
        lambda bases: None,
        (zero,) * (2 * PAIRS),
    )

    rows[pl.ds(me, 1)] = (row[...] + lanes_of(jnp.stack(sums), 0))[None]

    for k in range(count - 1):
        pltpu.make_async_remote_copy(
            src_ref=rows.at[me],
            dst_ref=rows.at[me],
            send_sem=sum_send.at[0],
            recv_sem=sum_recv.at[0],
            device_id={"gz": k + jnp.where(me <= k, 1, 0)},
            device_id_type=MESH,
        ).start()

    wait_sent(nxt)
    wait_sent(cur)

    others = rows.at[pl.ds(0, count - 1)]
    everyone = pltpu.make_async_remote_copy(
        src_ref=others,
        dst_ref=others,
        send_sem=sum_send.at[0],
        recv_sem=sum_recv.at[0],
        device_id={"gz": lax.rem(me + 1, count)},
        device_id_type=MESH,
    )
    everyone.wait_send()
    everyone.wait_recv()
    total[...] = jnp.sum(rows[...], axis=0)


def finish(
    final, grad, s_vec, y_vec, total, out_field, out_gradient, out_direction, result, sem
):
    def store(src, dst, h, group):
        pltpu.make_async_copy(src, dst.at[..., pl.ds(h * LANES, LANES)], sem.at[group]).start()

    for h in range(2):
        store(final.at[:, :, h], out_field, h, 0)
        store(grad.at[:, h], out_gradient, h, 1)

    nx = grad.shape[2]
    lane = lax.broadcasted_iota(jnp.int32, (1, LANES), 1)
    sums = total[...]

    def value(k):
        return jnp.sum(jnp.where(lane == k, sums, 0.0), axis=1, keepdims=True)

    sg = [value(k) for k in range(PAIRS)]
    yg = [value(PAIRS + k) for k in range(PAIRS)]
    pair = {}
    for w, (kind, a, b) in enumerate(WANTED):
        pair[kind, a, b] = value(2 * PAIRS + w)
        if kind == "yy":
            pair[kind, b, a] = pair[kind, a, b]
    rho = [1.0 / pair["sy", i, i] for i in range(PAIRS)]
    alphas = [None] * PAIRS
    for i in reversed(range(PAIRS)):
        dot = sg[i]
        for j in reversed(range(i + 1, PAIRS)):
            dot = dot - alphas[j] * pair["sy", i, j]
        alphas[i] = dot * rho[i]
    gamma = pair["sy", PAIRS - 1, PAIRS - 1] / pair["yy", PAIRS - 1, PAIRS - 1]
    extra = []
    for i in range(PAIRS):
        dot = yg[i]
        for j in range(PAIRS):
            dot = dot - alphas[j] * pair["yy", i, j]
        dot = gamma * dot
        for j in range(i):
            dot = dot + extra[j] * pair["sy", j, i]
        extra.append(alphas[i] - dot * rho[i])

    def wide(x):
        return jnp.broadcast_to(x, (8, LANES))

    of_g = wide(-gamma)
    of_y = [wide(gamma * alphas[i]) for i in range(PAIRS)]
    of_s = [wide(-extra[i]) for i in range(PAIRS)]
    for p in range(2):

        def combine(i, carry):
            at = pl.ds(pl.multiple_of(i * 8, 8), 8)
            for h in range(2):
                parts = [of_g * grad[p, h, at, :], of_s[0] * s_vec[0, p, h, at, :]]
                for k in range(PAIRS):
                    parts[0] = parts[0] + of_y[k] * y_vec[k, p, h, at, :]
                    if k > 0:
                        parts[1] = parts[1] + of_s[k] * s_vec[k, p, h, at, :]
                result[p, h, at, :] = parts[0] + parts[1]
            return carry

        lax.fori_loop(0, nx // 8, combine, 0, unroll=4)
        for h in range(2):
            store(result.at[p, h], out_direction.at[p], h, 2)
    for group, out in enumerate((out_field, out_gradient, out_direction)):
        pltpu.make_async_copy(out, out, sem.at[group]).wait()


def on_device(*args):
    now = args[0]
    lame = args[2]
    nx = now.shape[2]
    count = lax.axis_size("gz")
    padded = nx + 2 * PAD
    chunks = (nx - REST) // ROWS + 1
    f32 = jnp.float32
    hbm = pl.BlockSpec(memory_space=pltpu.HBM)
    vmem = pl.BlockSpec(memory_space=pltpu.VMEM)
    in_specs = [hbm] * 10
    plane = (2, 2, nx, LANES)
    halves = pl.pallas_call(
        kernel,
        out_shape=(
            jax.ShapeDtypeStruct((3, *plane), f32),
            jax.ShapeDtypeStruct(plane, f32),
            jax.ShapeDtypeStruct((PAIRS, *plane), f32),
            jax.ShapeDtypeStruct((PAIRS, *plane), f32),
            jax.ShapeDtypeStruct((1, LANES), f32),
        ),
        in_specs=in_specs,
        out_specs=(vmem,) * 5,
        scratch_shapes=[
            pltpu.SMEM((STEPS,), f32),
            pltpu.VMEM((2, 3, 2, 2, padded, LANES), f32),
            pltpu.VMEM((2, 2, 3, 2, padded, LANES), f32),
            pltpu.VMEM((7, *plane), f32),
            pltpu.VMEM((len(WANTED), 8, LANES), f32),
            pltpu.VMEM((1, LANES), f32),
            pltpu.VMEM((count, 1, LANES), f32),
            pltpu.SemaphoreType.DMA((2,)),
            pltpu.SemaphoreType.DMA((2, chunks)),
            pltpu.SemaphoreType.DMA((2,)),
            pltpu.SemaphoreType.DMA((2, 2)),
            pltpu.SemaphoreType.DMA((6,)),
            pltpu.SemaphoreType.REGULAR((3,)),
            pltpu.SemaphoreType.DMA((1,)),
            pltpu.SemaphoreType.DMA((1,)),
        ],
        compiler_params=pltpu.CompilerParams(
            collective_id=0, has_side_effects=True, vmem_limit_bytes=20 * 1024 * 1024
        ),
        name="leapfrog",
    )(*[pltpu.with_memory_space_constraint(x, pltpu.HBM) for x in args])
    return pl.pallas_call(
        finish,
        out_shape=(
            jax.ShapeDtypeStruct(now.shape, f32),
            jax.ShapeDtypeStruct(lame.shape, f32),
            jax.ShapeDtypeStruct(lame.shape, f32),
        ),
        in_specs=[vmem] * 5,
        out_specs=(hbm,) * 3,
        scratch_shapes=[pltpu.VMEM(plane, f32), pltpu.SemaphoreType.DMA((3,))],
        compiler_params=pltpu.CompilerParams(vmem_limit_bytes=8 * 1024 * 1024),
        name="finish",
    )(*halves)


def solution(mesh):
    placed = (
        P("sample", "gz", None, None),
        P("sample", "gz", None, None),
        P("gz", "sample", None),
        P("gz", "sample", None),
        P("gz", "sample", None),
        P("sample", "gz", None, None),
        P("sample"),
        P("gz", "sample", None),
        P("sample", "gz", None, None),
        P("sample", "gz", None, None),
    )
    return jax.shard_map(
        on_device,
        mesh=mesh,
        in_specs=placed,
        out_specs=(P("sample", "gz", None, None), P("gz", "sample", None), P("gz", "sample", None)),
        check_vma=False,
    )
```

```python
import jax
import jax.numpy as jnp
from jax import lax
from jax.experimental import pallas as pl
from jax.experimental.pallas import tpu as pltpu
from jax.sharding import PartitionSpec as P

STEPS = 8
PAIRS = 4
WANTED = [("sy", i, j) for i in range(PAIRS) for j in range(i, PAIRS)]
WANTED += [("yy", i, j) for i in range(PAIRS) for j in range(i, PAIRS)]
ROWS = 16
REST = 16
PAD = 8
LANES = 128
MESH = pl.DeviceIdType.MESH


def kernel(
    now, before, lame, shear, density, source, wave, prior, steps, changes,
    final, grad, s_vec, y_vec, total,
    wavelet, field, halo, bank, products, row, rows,
    link_send, link_recv, pair_send, pair_recv, load_sem, hello_sem, sum_send, sum_recv,
):
    me = lax.axis_index("gz")
    count = lax.axis_size("gz")
    nx = grad.shape[2]
    last = (nx - REST) // ROWS
    split = (last + 1) // 2
    padded = nx + 2 * PAD
    zero = jnp.zeros((8, LANES), jnp.float32)
    lane = lax.broadcasted_iota(jnp.int32, (8, LANES), 1)
    row_lane = lax.broadcasted_iota(jnp.int32, (1, LANES), 1)
    at_start = lane == 0
    at_end = lane == LANES - 1
    exists = (me > 0, me < count - 1)
    first_coef, second_coef, density_of, prior_of = (bank.at[k] for k in range(4))
    force = bank.at[pl.ds(4, 3)]

    core = lax.rem(me, 2)
    pair, link = 1 - core, core
    pair_peer = me + 1 - 2 * core
    linked = jnp.logical_and(me + 2 * core - 1 >= 0, me + 2 * core - 1 < count)
    link_peer = jnp.clip(me + 2 * core - 1, 0, count - 1)

    barrier = pltpu.get_barrier_semaphore()
    pl.semaphore_signal(barrier, inc=1, device_id={"gz": pair_peer}, device_id_type=MESH)

    @pl.when(linked)
    def _():
        pl.semaphore_signal(barrier, inc=1, device_id={"gz": link_peer}, device_id_type=MESH)

    inner = pl.ds(PAD, nx)

    def load(src, dst_of, group):
        for h in range(2):
            pltpu.make_async_copy(
                src.at[..., pl.ds(h * LANES, LANES)], dst_of(h), load_sem.at[group]
            ).start()

    def loaded(dst, group):
        pltpu.make_async_copy(dst, dst, load_sem.at[group]).wait()

    load(now, lambda h: field.at[0, :, :, h, inner, :], 0)

    for par in range(2):
        for c in range(3):
            for d in range(2):
                for h in range(2):
                    for edge in (0, padded - PAD):
                        field[par, c, d, h, edge : edge + 8, :] = zero
                        halo[par, d, c, h, edge : edge + 8, :] = zero
    for d in range(2):

        @pl.when(jnp.logical_not(exists[d]))
        def _():
            def clear(i, carry):
                at = pl.ds(pl.multiple_of(i * 8, 8), 8)
                for par in range(2):
                    for c in range(3):
                        for h in range(2):
                            halo[par, d, c, h, at, :] = zero
                return carry

            lax.fori_loop(0, padded // 8, clear, 0)

    pl.semaphore_wait(barrier, jnp.where(linked, 2, 1))

    def link_rows(j):
        if isinstance(j, int):
            return j * ROWS, REST if j == last else ROWS
        return pl.multiple_of(j * ROWS, 8), ROWS

    def pair_rows(i):
        return (split * ROWS, nx - split * ROWS) if i else (0, split * ROWS)

    def over_link(par, start, size, sem):
        at = pl.ds(PAD + start, size)
        return pltpu.make_async_remote_copy(
            src_ref=field.at[par, :, link, :, at, :],
            dst_ref=halo.at[par, 1 - link, :, :, at, :],
            send_sem=link_send.at[par],
            recv_sem=link_recv.at[par, sem],
            device_id={"gz": link_peer},
            device_id_type=MESH,
        )

    def to_pair(par, start, size, sem):
        at = pl.ds(PAD + start, size)
        return pltpu.make_async_remote_copy(
            src_ref=field.at[par, :, pair, :, at, :],
            dst_ref=halo.at[par, 1 - pair, :, :, at, :],
            send_sem=pair_send.at[par],
            recv_sem=pair_recv.at[par, sem],
            device_id={"gz": pair_peer},
            device_id_type=MESH,
        )

    def from_argument(direction, start, size, h, send_sem, recv_sem, peer):
        pltpu.make_async_remote_copy(
            src_ref=now.at[:, direction, pl.ds(start, size), pl.ds(h * LANES, LANES)],
            dst_ref=halo.at[0, 1 - direction, :, h, pl.ds(PAD + start, size), :],
            send_sem=send_sem,
            recv_sem=recv_sem,
            device_id={"gz": peer},
            device_id_type=MESH,
        ).start()

    def first_send(j, carry):
        for h in range(2):
            from_argument(
                link, *link_rows(j), h, link_send.at[0], link_recv.at[0, j], link_peer
            )
        return carry

    around = jnp.logical_and(linked, lax.rem(me + core, 8) == 0)

    @pl.when(jnp.logical_and(linked, jnp.logical_not(around)))
    def _():
        lax.fori_loop(0, last, first_send, 0)
        first_send(last, 0)

    @pl.when(around)
    def _():
        loaded(field.at[0, :, :, :, inner, :], 0)

        def loaded_send(j, carry):
            over_link(0, *link_rows(j), j).start()
            return carry

        lax.fori_loop(0, last, loaded_send, 0)
        over_link(0, *link_rows(last), last).start()

    for i in range(2):
        for h in range(2):
            from_argument(
                pair, *pair_rows(i), h, pair_send.at[0], pair_recv.at[0, i], pair_peer
            )
    wave_copy = pltpu.make_async_copy(wave, wavelet, load_sem.at[3])
    wave_copy.start()
    load(lame, lambda h: first_coef.at[:, h], 1)
    load(shear, lambda h: second_coef.at[:, h], 1)
    load(density, lambda h: density_of.at[:, h], 1)
    load(prior, lambda h: prior_of.at[:, h], 1)
    load(source, lambda h: force.at[:, :, h], 1)
    load(before, lambda h: field.at[1, :, :, h, inner, :], 2)

    def send_link(par, j):
        pl.when(linked)(lambda: over_link(par, *link_rows(j), j).start())

    def send_pair(par, i):
        to_pair(par, *pair_rows(i), i).start()

    def wait_sent(par):
        to_pair(par, 0, nx, 0).wait_send()
        pl.when(linked)(lambda: over_link(par, 0, nx, 0).wait_send())

    def wait_link(par, j):
        @pl.when(linked)
        def _():
            start, size = link_rows(j)
            at = pl.ds(PAD + start, size)
            pltpu.make_async_remote_copy(
                src_ref=field.at[par, :, link, :, at, :],
                dst_ref=halo.at[par, link, :, :, at, :],
                send_sem=link_send.at[par],
                recv_sem=link_recv.at[par, j],
                device_id={"gz": link_peer},
                device_id_type=MESH,
            ).wait_recv()

    def wait_pair(par, i):
        start, size = pair_rows(i)
        at = pl.ds(PAD + start, size)
        pltpu.make_async_remote_copy(
            src_ref=field.at[par, :, pair, :, at, :],
            dst_ref=halo.at[par, pair, :, :, at, :],
            send_sem=pair_send.at[par],
            recv_sem=pair_recv.at[par, i],
            device_id={"gz": pair_peer},
            device_id_type=MESH,
        ).wait_recv()

    rounds = []
    while 4 << len(rounds) < count:
        rounds.append(4 << len(rounds))

    def far(r, d):
        return me + rounds[r] if d else me - rounds[r]

    def within(r, d):
        return far(r, d) < count if d else far(r, d) >= 0

    def tell_far(r):
        for d in range(2):

            @pl.when(within(r, d))
            def _():
                pl.semaphore_signal(
                    hello_sem.at[r], inc=1, device_id={"gz": far(r, d)}, device_id_type=MESH
                )

    def hear_far(r):
        heard = jnp.where(within(r, 0), 1, 0) + jnp.where(within(r, 1), 1, 0)
        pl.when(heard > 0)(lambda: pl.semaphore_wait(hello_sem.at[r], heard))

    def acquaint(n):
        for r in range(len(rounds) + 1):

            @pl.when(n == 3 + r)
            def _():
                if r > 0:
                    hear_far(r - 1)
                if r < len(rounds):
                    tell_far(r)


    wave_copy.wait()
    loaded(bank, 1)
    pl.when(jnp.logical_not(around))(lambda: loaded(field.at[0, :, :, :, inner, :], 0))
    loaded(field.at[1, :, :, :, inner, :], 2)
    load(steps, lambda h: s_vec.at[:, :, h], 4)
    load(changes, lambda h: y_vec.at[:, :, h], 5)

    def prepare(i, carry):
        at = pl.ds(pl.multiple_of(i * 8, 8), 8)
        for p in range(2):
            for h in range(2):
                mu = second_coef[p, h, at, :]
                coeff = 0.04 / density_of[p, h, at, :]
                first_coef[p, h, at, :] = 0.25 * coeff * (first_coef[p, h, at, :] + mu)
                second_coef[p, h, at, :] = coeff * mu
                grad[p, h, at, :] = mu - prior_of[p, h, at, :]
                for c in range(3):
                    force[c, p, h, at, :] = coeff * force[c, p, h, at, :]
        return carry

    lax.fori_loop(0, nx // 8, prepare, 0)

    for w in range(len(WANTED)):
        products[w] = zero

    def gram(bases):
        for w, (kind, a, b) in enumerate(WANTED):
            part = products[w]
            for base in bases:
                at = pl.ds(base, 8)
                for p in range(2):
                    for h in range(2):
                        one = s_vec if kind == "sy" else y_vec
                        part = part + one[a, p, h, at, :] * y_vec[b, p, h, at, :]
            products[w] = part

    def lanes_of(x, first):
        n = x.shape[0]
        sums = jnp.sum(jnp.sum(x, axis=1), axis=1, keepdims=True)
        there = lax.broadcasted_iota(jnp.int32, (n, LANES), 1)
        wanted = lax.broadcasted_iota(jnp.int32, (n, LANES), 0) + first
        return jnp.sum(jnp.where(there == wanted, sums, 0.0), axis=0, keepdims=True)

    def along_y(v):
        back = [pltpu.roll(x, 1, 1) for x in v]
        ahead = [pltpu.roll(x, LANES - 1, 1) for x in v]
        plus = (jnp.where(at_end, ahead[1], ahead[0]), jnp.where(at_end, 0.0, ahead[1]))
        minus = (jnp.where(at_start, 0.0, back[0]), jnp.where(at_start, back[0], back[1]))
        return plus, minus

    def add(a, b):
        return (a[0] + b[0], a[1] + b[1])

    def sub(a, b):
        return (a[0] - b[0], a[1] - b[1])

    def block(cur, nxt, amplitude, base, out=None):
        at = pl.ds(base, 8)

        def rows_of(c, z, offset):
            from_row = pl.ds(base + PAD + offset, 8)
            if z in (-1, 2):
                return tuple(halo[cur, 0 if z < 0 else 1, c, h, from_row, :] for h in range(2))
            return tuple(field[cur, c, z, h, from_row, :] for h in range(2))

        u = {(c, z): rows_of(c, z, 0) for c in range(3) for z in (-1, 0, 1, 2)}
        up = {}
        down = {}
        for c in range(3):
            for z in (-1, 0, 1, 2) if c < 2 else (0, 1):
                up[c, z] = rows_of(c, z, 1)
                down[c, z] = rows_of(c, z, -1)
        dx = {key: sub(up[key], down[key]) for key in up}
        dy2 = {}
        sy = {}
        for z in (-1, 0, 1, 2):
            plus, minus = along_y(u[2, z])
            dy2[z] = sub(plus, minus)
            if z in (0, 1):
                sy[2, z] = add(plus, minus)
        mix0 = {z: add(dx[1, z], dy2[z]) for z in (-1, 0, 1, 2)}
        grads = []
        for z in range(2):
            for c in range(2):
                sy[c, z] = add(*along_y(u[c, z]))
            dz0 = sub(u[0, z + 1], u[0, z - 1])
            cross = [
                sub(mix0[z + 1], mix0[z - 1]),
                add(sub(dx[0, z + 1], dx[0, z - 1]), sub(*along_y(dx[2, z]))),
                sub(*along_y(add(dz0, dx[1, z]))),
            ]
            work = [None, None]
            for c in range(3):
                sz = add(u[c, z + 1], u[c, z - 1])
                sx = add(up[c, z], down[c, z])
                own = (sz, sx, sy[c, z])[c]
                for h in range(2):
                    centre = u[c, z][h]
                    twice = centre + centre
                    laplace = sz[h] + sx[h] + sy[c, z][h] - 6.0 * centre
                    div = 4.0 * (own[h] - twice) + cross[c][h]
                    new = (
                        twice
                        - field[nxt, c, z, h, pl.ds(base + PAD, 8), :]
                        + first_coef[z, h, at, :] * div
                        + second_coef[z, h, at, :] * laplace
                        + amplitude * force[c, z, h, at, :]
                    )
                    if out is None:
                        field[nxt, c, z, h, pl.ds(base + PAD, 8), :] = new
                    else:
                        out[c, z, h, at, :] = new
                    term = centre * laplace
                    work[h] = term if work[h] is None else work[h] + term
            for h in range(2):
                new = grad[z, h, at, :] + 0.02 * work[h]
                grad[z, h, at, :] = new
                grads.append((z, h, new))
        return grads

    def sweep(cur, nxt, amplitude, out, after, ending, carry):
        def at_split(j, act):
            if isinstance(j, int):
                if j == split:
                    act()
            else:
                pl.when(j == split)(act)

        def part(j, bases, carry):
            wait_link(cur, j)
            at_split(j, lambda: wait_pair(cur, 1))
            for i, base in enumerate(bases):
                carry = after(base, block(cur, nxt, amplitude, base, out), carry)
                if i == 0 and out is None and not (isinstance(j, int) and j == 0):
                    send_link(nxt, j - 1)
                    at_split(j, lambda: send_pair(nxt, 0))
            ending(bases)
            return carry

        def later(j, carry):
            return part(j, [pl.multiple_of(j * ROWS + k, 8) for k in range(-8, ROWS - 8, 8)], carry)

        wait_pair(cur, 0)
        carry = part(0, list(range(0, ROWS - 8, 8)), carry)
        carry = lax.fori_loop(1, last, later, carry)
        carry = part(last, [last * ROWS + k for k in range(-8, REST, 8)], carry)
        if out is None:
            send_link(nxt, last)
            send_pair(nxt, 1)
        return carry

    def step(n, carry):
        cur = lax.rem(n, 2)
        nxt = 1 - cur
        pl.when(n >= 1)(lambda: wait_sent(nxt))
        acquaint(n)

        @pl.when(n == 1)
        def _():
            loaded(s_vec, 4)
            loaded(y_vec, 5)

        @pl.when(n == 2)
        def _():
            row[...] = lanes_of(products[...], 2 * PAIRS)

        return sweep(
            cur,
            nxt,
            wavelet[n],
            None,
            lambda base, grads, carry: carry,
            lambda bases: pl.when(n == 1)(lambda: gram(bases)),
            carry,
        )

    lax.fori_loop(0, STEPS - 1, step, 0)

    cur, nxt = (STEPS - 1) % 2, STEPS % 2

    def multiply(base, grads, sums):
        sums = list(sums)
        for z, h, g in grads:
            for k in range(PAIRS):
                sums[k] = sums[k] + s_vec[k, z, h, pl.ds(base, 8), :] * g
                sums[PAIRS + k] = sums[PAIRS + k] + y_vec[k, z, h, pl.ds(base, 8), :] * g
        return tuple(sums)

    sums = sweep(
        cur,
        nxt,
        wavelet[STEPS - 1],
        final,
        multiply,
        lambda bases: None,
        (zero,) * (2 * PAIRS),
    )

    rows[pl.ds(me, 1)] = (row[...] + lanes_of(jnp.stack(sums), 0))[None]

    for k in range(count - 1):
        pltpu.make_async_remote_copy(
            src_ref=rows.at[me],
            dst_ref=rows.at[me],
            send_sem=sum_send.at[0],
            recv_sem=sum_recv.at[0],
            device_id={"gz": k + jnp.where(me <= k, 1, 0)},
            device_id_type=MESH,
        ).start()

    wait_sent(nxt)
    wait_sent(cur)

    others = rows.at[pl.ds(0, count - 1)]
    everyone = pltpu.make_async_remote_copy(
        src_ref=others,
        dst_ref=others,
        send_sem=sum_send.at[0],
        recv_sem=sum_recv.at[0],
        device_id={"gz": lax.rem(me + 1, count)},
        device_id_type=MESH,
    )
    everyone.wait_send()
    everyone.wait_recv()
    total[...] = jnp.sum(rows[...], axis=0)


def finish(
    final, grad, s_vec, y_vec, total, out_field, out_gradient, out_direction, result, sem
):
    def store(src, dst, h, group):
        pltpu.make_async_copy(src, dst.at[..., pl.ds(h * LANES, LANES)], sem.at[group]).start()

    for h in range(2):
        store(final.at[:, :, h], out_field, h, 0)
        store(grad.at[:, h], out_gradient, h, 1)

    nx = grad.shape[2]
    lane = lax.broadcasted_iota(jnp.int32, (1, LANES), 1)
    sums = total[...]

    def value(k):
        return jnp.sum(jnp.where(lane == k, sums, 0.0), axis=1, keepdims=True)

    sg = [value(k) for k in range(PAIRS)]
    yg = [value(PAIRS + k) for k in range(PAIRS)]
    pair = {}
    for w, (kind, a, b) in enumerate(WANTED):
        pair[kind, a, b] = value(2 * PAIRS + w)
        if kind == "yy":
            pair[kind, b, a] = pair[kind, a, b]
    rho = [1.0 / pair["sy", i, i] for i in range(PAIRS)]
    alphas = [None] * PAIRS
    for i in reversed(range(PAIRS)):
        dot = sg[i]
        for j in reversed(range(i + 1, PAIRS)):
            dot = dot - alphas[j] * pair["sy", i, j]
        alphas[i] = dot * rho[i]
    gamma = pair["sy", PAIRS - 1, PAIRS - 1] / pair["yy", PAIRS - 1, PAIRS - 1]
    extra = []
    for i in range(PAIRS):
        dot = yg[i]
        for j in range(PAIRS):
            dot = dot - alphas[j] * pair["yy", i, j]
        dot = gamma * dot
        for j in range(i):
            dot = dot + extra[j] * pair["sy", j, i]
        extra.append(alphas[i] - dot * rho[i])

    def wide(x):
        return jnp.broadcast_to(x, (8, LANES))

    of_g = wide(-gamma)
    of_y = [wide(gamma * alphas[i]) for i in range(PAIRS)]
    of_s = [wide(-extra[i]) for i in range(PAIRS)]
    for p in range(2):

        def combine(i, carry):
            at = pl.ds(pl.multiple_of(i * 8, 8), 8)
            for h in range(2):
                parts = [of_g * grad[p, h, at, :], of_s[0] * s_vec[0, p, h, at, :]]
                for k in range(PAIRS):
                    parts[0] = parts[0] + of_y[k] * y_vec[k, p, h, at, :]
                    if k > 0:
                        parts[1] = parts[1] + of_s[k] * s_vec[k, p, h, at, :]
                result[p, h, at, :] = parts[0] + parts[1]
            return carry

        lax.fori_loop(0, nx // 8, combine, 0, unroll=4)
        for h in range(2):
            store(result.at[p, h], out_direction.at[p], h, 2)
    for group, out in enumerate((out_field, out_gradient, out_direction)):
        pltpu.make_async_copy(out, out, sem.at[group]).wait()


def on_device(*args):
    now = args[0]
    lame = args[2]
    nx = now.shape[2]
    count = lax.axis_size("gz")
    padded = nx + 2 * PAD
    chunks = (nx - REST) // ROWS + 1
    f32 = jnp.float32
    hbm = pl.BlockSpec(memory_space=pltpu.HBM)
    vmem = pl.BlockSpec(memory_space=pltpu.VMEM)
    in_specs = [hbm] * 10
    plane = (2, 2, nx, LANES)
    halves = pl.pallas_call(
        kernel,
        out_shape=(
            jax.ShapeDtypeStruct((3, *plane), f32),
            jax.ShapeDtypeStruct(plane, f32),
            jax.ShapeDtypeStruct((PAIRS, *plane), f32),
            jax.ShapeDtypeStruct((PAIRS, *plane), f32),
            jax.ShapeDtypeStruct((1, LANES), f32),
        ),
        in_specs=in_specs,
        out_specs=(vmem,) * 5,
        scratch_shapes=[
            pltpu.SMEM((STEPS,), f32),
            pltpu.VMEM((2, 3, 2, 2, padded, LANES), f32),
            pltpu.VMEM((2, 2, 3, 2, padded, LANES), f32),
            pltpu.VMEM((7, *plane), f32),
            pltpu.VMEM((len(WANTED), 8, LANES), f32),
            pltpu.VMEM((1, LANES), f32),
            pltpu.VMEM((count, 1, LANES), f32),
            pltpu.SemaphoreType.DMA((2,)),
            pltpu.SemaphoreType.DMA((2, chunks)),
            pltpu.SemaphoreType.DMA((2,)),
            pltpu.SemaphoreType.DMA((2, 2)),
            pltpu.SemaphoreType.DMA((6,)),
            pltpu.SemaphoreType.REGULAR((3,)),
            pltpu.SemaphoreType.DMA((1,)),
            pltpu.SemaphoreType.DMA((1,)),
        ],
        compiler_params=pltpu.CompilerParams(
            collective_id=0, has_side_effects=True, vmem_limit_bytes=20 * 1024 * 1024
        ),
        name="leapfrog",
    )(*[pltpu.with_memory_space_constraint(x, pltpu.HBM) for x in args])
    return pl.pallas_call(
        finish,
        out_shape=(
            jax.ShapeDtypeStruct(now.shape, f32),
            jax.ShapeDtypeStruct(lame.shape, f32),
            jax.ShapeDtypeStruct(lame.shape, f32),
        ),
        in_specs=[vmem] * 5,
        out_specs=(hbm,) * 3,
        scratch_shapes=[pltpu.VMEM(plane, f32), pltpu.SemaphoreType.DMA((3,))],
        compiler_params=pltpu.CompilerParams(vmem_limit_bytes=8 * 1024 * 1024),
        name="finish",
    )(*halves)


def solution(mesh):
    placed = (
        P("sample", "gz", None, None),
        P("sample", "gz", None, None),
        P("gz", "sample", None),
        P("gz", "sample", None),
        P("gz", "sample", None),
        P("sample", "gz", None, None),
        P("sample"),
        P("gz", "sample", None),
        P("sample", "gz", None, None),
        P("sample", "gz", None, None),
    )
    return jax.shard_map(
        on_device,
        mesh=mesh,
        in_specs=placed,
        out_specs=(P("sample", "gz", None, None), P("gz", "sample", None), P("gz", "sample", None)),
        check_vma=False,
    )
```

```python
import jax
import jax.numpy as jnp
from jax import lax
from jax.experimental import pallas as pl
from jax.experimental.pallas import tpu as pltpu
from jax.sharding import PartitionSpec as P

STEPS = 8
PAIRS = 4
WANTED = [("sy", i, j) for i in range(PAIRS) for j in range(i, PAIRS)]
WANTED += [("yy", i, j) for i in range(PAIRS) for j in range(i, PAIRS)]
ROWS = 16
REST = 16
PAD = 8
LANES = 128
MESH = pl.DeviceIdType.MESH


def kernel(
    now, before, lame, shear, density, source, wave, prior, steps, changes,
    final, grad, s_vec, y_vec, total,
    wavelet, field, halo, bank, products, row, rows,
    link_send, link_recv, pair_send, pair_recv, load_sem, hello_sem, sum_send, sum_recv,
):
    me = lax.axis_index("gz")
    count = lax.axis_size("gz")
    nx = grad.shape[2]
    last = (nx - REST) // ROWS
    split = (last + 1) // 2
    padded = nx + 2 * PAD
    zero = jnp.zeros((8, LANES), jnp.float32)
    lane = lax.broadcasted_iota(jnp.int32, (8, LANES), 1)
    row_lane = lax.broadcasted_iota(jnp.int32, (1, LANES), 1)
    at_start = lane == 0
    at_end = lane == LANES - 1
    exists = (me > 0, me < count - 1)
    first_coef, second_coef, density_of, prior_of = (bank.at[k] for k in range(4))
    force = bank.at[pl.ds(4, 3)]

    core = lax.rem(me, 2)
    pair, link = 1 - core, core
    pair_peer = me + 1 - 2 * core
    linked = jnp.logical_and(me + 2 * core - 1 >= 0, me + 2 * core - 1 < count)
    link_peer = jnp.clip(me + 2 * core - 1, 0, count - 1)

    barrier = pltpu.get_barrier_semaphore()
    pl.semaphore_signal(barrier, inc=1, device_id={"gz": pair_peer}, device_id_type=MESH)

    @pl.when(linked)
    def _():
        pl.semaphore_signal(barrier, inc=1, device_id={"gz": link_peer}, device_id_type=MESH)

    inner = pl.ds(PAD, nx)

    def load(src, dst_of, group):
        for h in range(2):
            pltpu.make_async_copy(
                src.at[..., pl.ds(h * LANES, LANES)], dst_of(h), load_sem.at[group]
            ).start()

    def loaded(dst, group):
        pltpu.make_async_copy(dst, dst, load_sem.at[group]).wait()

    load(now, lambda h: field.at[0, :, :, h, inner, :], 0)

    for par in range(2):
        for c in range(3):
            for d in range(2):
                for h in range(2):
                    for edge in (0, padded - PAD):
                        field[par, c, d, h, edge : edge + 8, :] = zero
                        halo[par, d, c, h, edge : edge + 8, :] = zero
    for d in range(2):

        @pl.when(jnp.logical_not(exists[d]))
        def _():
            def clear(i, carry):
                at = pl.ds(pl.multiple_of(i * 8, 8), 8)
                for par in range(2):
                    for c in range(3):
                        for h in range(2):
                            halo[par, d, c, h, at, :] = zero
                return carry

            lax.fori_loop(0, padded // 8, clear, 0)

    pl.semaphore_wait(barrier, jnp.where(linked, 2, 1))

    def link_rows(j):
        if isinstance(j, int):
            return j * ROWS, REST if j == last else ROWS
        return pl.multiple_of(j * ROWS, 8), ROWS

    def pair_rows(i):
        return (split * ROWS, nx - split * ROWS) if i else (0, split * ROWS)

    def over_link(par, start, size, sem):
        at = pl.ds(PAD + start, size)
        return pltpu.make_async_remote_copy(
            src_ref=field.at[par, :, link, :, at, :],
            dst_ref=halo.at[par, 1 - link, :, :, at, :],
            send_sem=link_send.at[par],
            recv_sem=link_recv.at[par, sem],
            device_id={"gz": link_peer},
            device_id_type=MESH,
        )

    def to_pair(par, start, size, sem):
        at = pl.ds(PAD + start, size)
        return pltpu.make_async_remote_copy(
            src_ref=field.at[par, :, pair, :, at, :],
            dst_ref=halo.at[par, 1 - pair, :, :, at, :],
            send_sem=pair_send.at[par],
            recv_sem=pair_recv.at[par, sem],
            device_id={"gz": pair_peer},
            device_id_type=MESH,
        )

    def from_argument(direction, start, size, h, send_sem, recv_sem, peer):
        pltpu.make_async_remote_copy(
            src_ref=now.at[:, direction, pl.ds(start, size), pl.ds(h * LANES, LANES)],
            dst_ref=halo.at[0, 1 - direction, :, h, pl.ds(PAD + start, size), :],
            send_sem=send_sem,
            recv_sem=recv_sem,
            device_id={"gz": peer},
            device_id_type=MESH,
        ).start()

    def first_send(j, carry):
        for h in range(2):
            from_argument(
                link, *link_rows(j), h, link_send.at[0], link_recv.at[0, j], link_peer
            )
        return carry

    around = jnp.logical_and(linked, lax.rem(me + core, 8) == 0)

    @pl.when(jnp.logical_and(linked, jnp.logical_not(around)))
    def _():
        lax.fori_loop(0, last, first_send, 0)
        first_send(last, 0)

    @pl.when(around)
    def _():
        loaded(field.at[0, :, :, :, inner, :], 0)

        def loaded_send(j, carry):
            over_link(0, *link_rows(j), j).start()
            return carry

        lax.fori_loop(0, last, loaded_send, 0)
        over_link(0, *link_rows(last), last).start()

    for i in range(2):
        for h in range(2):
            from_argument(
                pair, *pair_rows(i), h, pair_send.at[0], pair_recv.at[0, i], pair_peer
            )
    wave_copy = pltpu.make_async_copy(wave, wavelet, load_sem.at[3])
    wave_copy.start()
    load(lame, lambda h: first_coef.at[:, h], 1)
    load(shear, lambda h: second_coef.at[:, h], 1)
    load(density, lambda h: density_of.at[:, h], 1)
    load(prior, lambda h: prior_of.at[:, h], 1)
    load(source, lambda h: force.at[:, :, h], 1)
    load(before, lambda h: field.at[1, :, :, h, inner, :], 2)

    def send_link(par, j):
        pl.when(linked)(lambda: over_link(par, *link_rows(j), j).start())

    def send_pair(par, i):
        to_pair(par, *pair_rows(i), i).start()

    def wait_sent(par):
        to_pair(par, 0, nx, 0).wait_send()
        pl.when(linked)(lambda: over_link(par, 0, nx, 0).wait_send())

    def wait_link(par, j):
        @pl.when(linked)
        def _():
            start, size = link_rows(j)
            at = pl.ds(PAD + start, size)
            pltpu.make_async_remote_copy(
                src_ref=field.at[par, :, link, :, at, :],
                dst_ref=halo.at[par, link, :, :, at, :],
                send_sem=link_send.at[par],
                recv_sem=link_recv.at[par, j],
                device_id={"gz": link_peer},
                device_id_type=MESH,
            ).wait_recv()

    def wait_pair(par, i):
        start, size = pair_rows(i)
        at = pl.ds(PAD + start, size)
        pltpu.make_async_remote_copy(
            src_ref=field.at[par, :, pair, :, at, :],
            dst_ref=halo.at[par, pair, :, :, at, :],
            send_sem=pair_send.at[par],
            recv_sem=pair_recv.at[par, i],
            device_id={"gz": pair_peer},
            device_id_type=MESH,
        ).wait_recv()

    rounds = []
    while 4 << len(rounds) < count:
        rounds.append(4 << len(rounds))

    def far(r, d):
        return me + rounds[r] if d else me - rounds[r]

    def within(r, d):
        return far(r, d) < count if d else far(r, d) >= 0

    def tell_far(r):
        for d in range(2):

            @pl.when(within(r, d))
            def _():
                pl.semaphore_signal(
                    hello_sem.at[r], inc=1, device_id={"gz": far(r, d)}, device_id_type=MESH
                )

    def hear_far(r):
        heard = jnp.where(within(r, 0), 1, 0) + jnp.where(within(r, 1), 1, 0)
        pl.when(heard > 0)(lambda: pl.semaphore_wait(hello_sem.at[r], heard))

    def acquaint(n):
        for r in range(len(rounds) + 1):

            @pl.when(n == 3 + r)
            def _():
                if r > 0:
                    hear_far(r - 1)
                if r < len(rounds):
                    tell_far(r)


    wave_copy.wait()
    loaded(bank, 1)
    pl.when(jnp.logical_not(around))(lambda: loaded(field.at[0, :, :, :, inner, :], 0))
    loaded(field.at[1, :, :, :, inner, :], 2)
    load(steps, lambda h: s_vec.at[:, :, h], 4)
    load(changes, lambda h: y_vec.at[:, :, h], 5)

    def prepare(i, carry):
        at = pl.ds(pl.multiple_of(i * 8, 8), 8)
        for p in range(2):
            for h in range(2):
                mu = second_coef[p, h, at, :]
                coeff = 0.04 / density_of[p, h, at, :]
                first_coef[p, h, at, :] = 0.25 * coeff * (first_coef[p, h, at, :] + mu)
                second_coef[p, h, at, :] = coeff * mu
                grad[p, h, at, :] = mu - prior_of[p, h, at, :]
                for c in range(3):
                    force[c, p, h, at, :] = coeff * force[c, p, h, at, :]
        return carry

    lax.fori_loop(0, nx // 8, prepare, 0)

    for w in range(len(WANTED)):
        products[w] = zero

    def gram(bases):
        for w, (kind, a, b) in enumerate(WANTED):
            part = products[w]
            for base in bases:
                at = pl.ds(base, 8)
                for p in range(2):
                    for h in range(2):
                        one = s_vec if kind == "sy" else y_vec
                        part = part + one[a, p, h, at, :] * y_vec[b, p, h, at, :]
            products[w] = part

    def lanes_of(x, first):
        n = x.shape[0]
        sums = jnp.sum(jnp.sum(x, axis=1), axis=1, keepdims=True)
        there = lax.broadcasted_iota(jnp.int32, (n, LANES), 1)
        wanted = lax.broadcasted_iota(jnp.int32, (n, LANES), 0) + first
        return jnp.sum(jnp.where(there == wanted, sums, 0.0), axis=0, keepdims=True)

    def along_y(v):
        back = [pltpu.roll(x, 1, 1) for x in v]
        ahead = [pltpu.roll(x, LANES - 1, 1) for x in v]
        plus = (jnp.where(at_end, ahead[1], ahead[0]), jnp.where(at_end, 0.0, ahead[1]))
        minus = (jnp.where(at_start, 0.0, back[0]), jnp.where(at_start, back[0], back[1]))
        return plus, minus

    def add(a, b):
        return (a[0] + b[0], a[1] + b[1])

    def sub(a, b):
        return (a[0] - b[0], a[1] - b[1])

    def block(cur, nxt, amplitude, base, out=None):
        at = pl.ds(base, 8)

        def rows_of(c, z, offset):
            from_row = pl.ds(base + PAD + offset, 8)
            if z in (-1, 2):
                return tuple(halo[cur, 0 if z < 0 else 1, c, h, from_row, :] for h in range(2))
            return tuple(field[cur, c, z, h, from_row, :] for h in range(2))

        u = {(c, z): rows_of(c, z, 0) for c in range(3) for z in (-1, 0, 1, 2)}
        up = {}
        down = {}
        for c in range(3):
            for z in (-1, 0, 1, 2) if c < 2 else (0, 1):
                up[c, z] = rows_of(c, z, 1)
                down[c, z] = rows_of(c, z, -1)
        dx = {key: sub(up[key], down[key]) for key in up}
        dy2 = {}
        sy = {}
        for z in (-1, 0, 1, 2):
            plus, minus = along_y(u[2, z])
            dy2[z] = sub(plus, minus)
            if z in (0, 1):
                sy[2, z] = add(plus, minus)
        mix0 = {z: add(dx[1, z], dy2[z]) for z in (-1, 0, 1, 2)}
        grads = []
        for z in range(2):
            for c in range(2):
                sy[c, z] = add(*along_y(u[c, z]))
            dz0 = sub(u[0, z + 1], u[0, z - 1])
            cross = [
                sub(mix0[z + 1], mix0[z - 1]),
                add(sub(dx[0, z + 1], dx[0, z - 1]), sub(*along_y(dx[2, z]))),
                sub(*along_y(add(dz0, dx[1, z]))),
            ]
            work = [None, None]
            for c in range(3):
                sz = add(u[c, z + 1], u[c, z - 1])
                sx = add(up[c, z], down[c, z])
                own = (sz, sx, sy[c, z])[c]
                for h in range(2):
                    centre = u[c, z][h]
                    twice = centre + centre
                    laplace = sz[h] + sx[h] + sy[c, z][h] - 6.0 * centre
                    div = 4.0 * (own[h] - twice) + cross[c][h]
                    new = (
                        twice
                        - field[nxt, c, z, h, pl.ds(base + PAD, 8), :]
                        + first_coef[z, h, at, :] * div
                        + second_coef[z, h, at, :] * laplace
                        + amplitude * force[c, z, h, at, :]
                    )
                    if out is None:
                        field[nxt, c, z, h, pl.ds(base + PAD, 8), :] = new
                    else:
                        out[c, z, h, at, :] = new
                    term = centre * laplace
                    work[h] = term if work[h] is None else work[h] + term
            for h in range(2):
                new = grad[z, h, at, :] + 0.02 * work[h]
                grad[z, h, at, :] = new
                grads.append((z, h, new))
        return grads

    def sweep(cur, nxt, amplitude, out, after, ending, carry):
        def at_split(j, act):
            if isinstance(j, int):
                if j == split:
                    act()
            else:
                pl.when(j == split)(act)

        def part(j, bases, carry):
            wait_link(cur, j)
            at_split(j, lambda: wait_pair(cur, 1))
            for i, base in enumerate(bases):
                carry = after(base, block(cur, nxt, amplitude, base, out), carry)
                if i == 0 and out is None and not (isinstance(j, int) and j == 0):
                    send_link(nxt, j - 1)
                    at_split(j, lambda: send_pair(nxt, 0))
            ending(bases)
            return carry

        def later(j, carry):
            return part(j, [pl.multiple_of(j * ROWS + k, 8) for k in range(-8, ROWS - 8, 8)], carry)

        wait_pair(cur, 0)
        carry = part(0, list(range(0, ROWS - 8, 8)), carry)
        carry = lax.fori_loop(1, last, later, carry)
        carry = part(last, [last * ROWS + k for k in range(-8, REST, 8)], carry)
        if out is None:
            send_link(nxt, last)
            send_pair(nxt, 1)
        return carry

    def step(n, cur, carry):
        nxt = 1 - cur
        pl.when(n >= 1)(lambda: wait_sent(nxt))
        acquaint(n)

        @pl.when(n == 1)
        def _():
            loaded(s_vec, 4)
            loaded(y_vec, 5)

        @pl.when(n == 2)
        def _():
            row[...] = lanes_of(products[...], 2 * PAIRS)

        return sweep(
            cur,
            nxt,
            wavelet[n],
            None,
            lambda base, grads, carry: carry,
            lambda bases: pl.when(n == 1)(lambda: gram(bases)),
            carry,
        )

    def two_steps(k, carry):
        return step(2 * k + 1, 1, step(2 * k, 0, carry))

    lax.fori_loop(0, STEPS // 2 - 1, two_steps, 0)
    lax.fori_loop(STEPS // 2 - 1, STEPS // 2, lambda k, carry: step(2 * k, 0, carry), 0)

    cur, nxt = (STEPS - 1) % 2, STEPS % 2

    def multiply(base, grads, sums):
        sums = list(sums)
        for z, h, g in grads:
            for k in range(PAIRS):
                sums[k] = sums[k] + s_vec[k, z, h, pl.ds(base, 8), :] * g
                sums[PAIRS + k] = sums[PAIRS + k] + y_vec[k, z, h, pl.ds(base, 8), :] * g
        return tuple(sums)

    sums = sweep(
        cur,
        nxt,
        wavelet[STEPS - 1],
        final,
        multiply,
        lambda bases: None,
        (zero,) * (2 * PAIRS),
    )

    rows[pl.ds(me, 1)] = (row[...] + lanes_of(jnp.stack(sums), 0))[None]

    for k in range(count - 1):
        pltpu.make_async_remote_copy(
            src_ref=rows.at[me],
            dst_ref=rows.at[me],
            send_sem=sum_send.at[0],
            recv_sem=sum_recv.at[0],
            device_id={"gz": k + jnp.where(me <= k, 1, 0)},
            device_id_type=MESH,
        ).start()

    wait_sent(nxt)
    wait_sent(cur)

    others = rows.at[pl.ds(0, count - 1)]
    everyone = pltpu.make_async_remote_copy(
        src_ref=others,
        dst_ref=others,
        send_sem=sum_send.at[0],
        recv_sem=sum_recv.at[0],
        device_id={"gz": lax.rem(me + 1, count)},
        device_id_type=MESH,
    )
    everyone.wait_send()
    everyone.wait_recv()
    total[...] = jnp.sum(rows[...], axis=0)


def finish(
    final, grad, s_vec, y_vec, total, out_field, out_gradient, out_direction, result, sem
):
    def store(src, dst, h, group):
        pltpu.make_async_copy(src, dst.at[..., pl.ds(h * LANES, LANES)], sem.at[group]).start()

    for h in range(2):
        store(final.at[:, :, h], out_field, h, 0)
        store(grad.at[:, h], out_gradient, h, 1)

    nx = grad.shape[2]
    lane = lax.broadcasted_iota(jnp.int32, (1, LANES), 1)
    sums = total[...]

    def value(k):
        return jnp.sum(jnp.where(lane == k, sums, 0.0), axis=1, keepdims=True)

    sg = [value(k) for k in range(PAIRS)]
    yg = [value(PAIRS + k) for k in range(PAIRS)]
    pair = {}
    for w, (kind, a, b) in enumerate(WANTED):
        pair[kind, a, b] = value(2 * PAIRS + w)
        if kind == "yy":
            pair[kind, b, a] = pair[kind, a, b]
    rho = [1.0 / pair["sy", i, i] for i in range(PAIRS)]
    alphas = [None] * PAIRS
    for i in reversed(range(PAIRS)):
        dot = sg[i]
        for j in reversed(range(i + 1, PAIRS)):
            dot = dot - alphas[j] * pair["sy", i, j]
        alphas[i] = dot * rho[i]
    gamma = pair["sy", PAIRS - 1, PAIRS - 1] / pair["yy", PAIRS - 1, PAIRS - 1]
    extra = []
    for i in range(PAIRS):
        dot = yg[i]
        for j in range(PAIRS):
            dot = dot - alphas[j] * pair["yy", i, j]
        dot = gamma * dot
        for j in range(i):
            dot = dot + extra[j] * pair["sy", j, i]
        extra.append(alphas[i] - dot * rho[i])

    def wide(x):
        return jnp.broadcast_to(x, (8, LANES))

    of_g = wide(-gamma)
    of_y = [wide(gamma * alphas[i]) for i in range(PAIRS)]
    of_s = [wide(-extra[i]) for i in range(PAIRS)]
    for p in range(2):

        def combine(i, carry):
            at = pl.ds(pl.multiple_of(i * 8, 8), 8)
            for h in range(2):
                parts = [of_g * grad[p, h, at, :], of_s[0] * s_vec[0, p, h, at, :]]
                for k in range(PAIRS):
                    parts[0] = parts[0] + of_y[k] * y_vec[k, p, h, at, :]
                    if k > 0:
                        parts[1] = parts[1] + of_s[k] * s_vec[k, p, h, at, :]
                result[p, h, at, :] = parts[0] + parts[1]
            return carry

        lax.fori_loop(0, nx // 8, combine, 0, unroll=4)
        for h in range(2):
            store(result.at[p, h], out_direction.at[p], h, 2)
    for group, out in enumerate((out_field, out_gradient, out_direction)):
        pltpu.make_async_copy(out, out, sem.at[group]).wait()


def on_device(*args):
    now = args[0]
    lame = args[2]
    nx = now.shape[2]
    count = lax.axis_size("gz")
    padded = nx + 2 * PAD
    chunks = (nx - REST) // ROWS + 1
    f32 = jnp.float32
    hbm = pl.BlockSpec(memory_space=pltpu.HBM)
    vmem = pl.BlockSpec(memory_space=pltpu.VMEM)
    in_specs = [hbm] * 10
    plane = (2, 2, nx, LANES)
    halves = pl.pallas_call(
        kernel,
        out_shape=(
            jax.ShapeDtypeStruct((3, *plane), f32),
            jax.ShapeDtypeStruct(plane, f32),
            jax.ShapeDtypeStruct((PAIRS, *plane), f32),
            jax.ShapeDtypeStruct((PAIRS, *plane), f32),
            jax.ShapeDtypeStruct((1, LANES), f32),
        ),
        in_specs=in_specs,
        out_specs=(vmem,) * 5,
        scratch_shapes=[
            pltpu.SMEM((STEPS,), f32),
            pltpu.VMEM((2, 3, 2, 2, padded, LANES), f32),
            pltpu.VMEM((2, 2, 3, 2, padded, LANES), f32),
            pltpu.VMEM((7, *plane), f32),
            pltpu.VMEM((len(WANTED), 8, LANES), f32),
            pltpu.VMEM((1, LANES), f32),
            pltpu.VMEM((count, 1, LANES), f32),
            pltpu.SemaphoreType.DMA((2,)),
            pltpu.SemaphoreType.DMA((2, chunks)),
            pltpu.SemaphoreType.DMA((2,)),
            pltpu.SemaphoreType.DMA((2, 2)),
            pltpu.SemaphoreType.DMA((6,)),
            pltpu.SemaphoreType.REGULAR((3,)),
            pltpu.SemaphoreType.DMA((1,)),
            pltpu.SemaphoreType.DMA((1,)),
        ],
        compiler_params=pltpu.CompilerParams(
            collective_id=0, has_side_effects=True, vmem_limit_bytes=20 * 1024 * 1024
        ),
        name="leapfrog",
    )(*[pltpu.with_memory_space_constraint(x, pltpu.HBM) for x in args])
    return pl.pallas_call(
        finish,
        out_shape=(
            jax.ShapeDtypeStruct(now.shape, f32),
            jax.ShapeDtypeStruct(lame.shape, f32),
            jax.ShapeDtypeStruct(lame.shape, f32),
        ),
        in_specs=[vmem] * 5,
        out_specs=(hbm,) * 3,
        scratch_shapes=[pltpu.VMEM(plane, f32), pltpu.SemaphoreType.DMA((3,))],
        compiler_params=pltpu.CompilerParams(vmem_limit_bytes=8 * 1024 * 1024),
        name="finish",
    )(*halves)


def solution(mesh):
    placed = (
        P("sample", "gz", None, None),
        P("sample", "gz", None, None),
        P("gz", "sample", None),
        P("gz", "sample", None),
        P("gz", "sample", None),
        P("sample", "gz", None, None),
        P("sample"),
        P("gz", "sample", None),
        P("sample", "gz", None, None),
        P("sample", "gz", None, None),
    )
    return jax.shard_map(
        on_device,
        mesh=mesh,
        in_specs=placed,
        out_specs=(P("sample", "gz", None, None), P("gz", "sample", None), P("gz", "sample", None)),
        check_vma=False,
    )
```

```python
import jax
import jax.numpy as jnp
from jax import lax
from jax.experimental import pallas as pl
from jax.experimental.pallas import tpu as pltpu
from jax.sharding import PartitionSpec as P

STEPS = 8
PAIRS = 4
WANTED = [("sy", i, j) for i in range(PAIRS) for j in range(i, PAIRS)]
WANTED += [("yy", i, j) for i in range(PAIRS) for j in range(i, PAIRS)]
ROWS = 16
REST = 16
PAD = 8
LANES = 128
MESH = pl.DeviceIdType.MESH


def kernel(
    now, before, lame, shear, density, source, wave, prior, steps, changes,
    final, grad, s_vec, y_vec, total,
    wavelet, field, halo, bank, products, row, rows,
    link_send, link_recv, pair_send, pair_recv, load_sem, hello_sem, sum_send, sum_recv,
):
    me = lax.axis_index("gz")
    count = lax.axis_size("gz")
    nx = grad.shape[2]
    last = (nx - REST) // ROWS
    split = (last + 1) // 2
    padded = nx + 2 * PAD
    zero = jnp.zeros((8, LANES), jnp.float32)
    lane = lax.broadcasted_iota(jnp.int32, (8, LANES), 1)
    row_lane = lax.broadcasted_iota(jnp.int32, (1, LANES), 1)
    at_start = lane == 0
    at_end = lane == LANES - 1
    exists = (me > 0, me < count - 1)
    first_coef, second_coef, density_of, prior_of = (bank.at[k] for k in range(4))
    force = bank.at[pl.ds(4, 3)]

    core = lax.rem(me, 2)
    pair, link = 1 - core, core
    pair_peer = me + 1 - 2 * core
    linked = jnp.logical_and(me + 2 * core - 1 >= 0, me + 2 * core - 1 < count)
    link_peer = jnp.clip(me + 2 * core - 1, 0, count - 1)

    barrier = pltpu.get_barrier_semaphore()

    @pl.when(linked)
    def _():
        pl.semaphore_signal(barrier, inc=1, device_id={"gz": link_peer}, device_id_type=MESH)

    pl.semaphore_signal(barrier, inc=1, device_id={"gz": pair_peer}, device_id_type=MESH)

    inner = pl.ds(PAD, nx)

    def load(src, dst_of, group):
        for h in range(2):
            pltpu.make_async_copy(
                src.at[..., pl.ds(h * LANES, LANES)], dst_of(h), load_sem.at[group]
            ).start()

    def loaded(dst, group):
        pltpu.make_async_copy(dst, dst, load_sem.at[group]).wait()

    load(now, lambda h: field.at[0, :, :, h, inner, :], 0)

    for par in range(2):
        for c in range(3):
            for d in range(2):
                for h in range(2):
                    for edge in (0, padded - PAD):
                        field[par, c, d, h, edge : edge + 8, :] = zero
                        halo[par, d, c, h, edge : edge + 8, :] = zero
    for d in range(2):

        @pl.when(jnp.logical_not(exists[d]))
        def _():
            def clear(i, carry):
                at = pl.ds(pl.multiple_of(i * 8, 8), 8)
                for par in range(2):
                    for c in range(3):
                        for h in range(2):
                            halo[par, d, c, h, at, :] = zero
                return carry

            lax.fori_loop(0, padded // 8, clear, 0)

    pl.semaphore_wait(barrier, jnp.where(linked, 2, 1))

    def link_rows(j):
        if isinstance(j, int):
            return j * ROWS, REST if j == last else ROWS
        return pl.multiple_of(j * ROWS, 8), ROWS

    def pair_rows(i):
        return (split * ROWS, nx - split * ROWS) if i else (0, split * ROWS)

    def over_link(par, start, size, sem):
        at = pl.ds(PAD + start, size)
        return pltpu.make_async_remote_copy(
            src_ref=field.at[par, :, link, :, at, :],
            dst_ref=halo.at[par, 1 - link, :, :, at, :],
            send_sem=link_send.at[par],
            recv_sem=link_recv.at[par, sem],
            device_id={"gz": link_peer},
            device_id_type=MESH,
        )

    def to_pair(par, start, size, sem):
        at = pl.ds(PAD + start, size)
        return pltpu.make_async_remote_copy(
            src_ref=field.at[par, :, pair, :, at, :],
            dst_ref=halo.at[par, 1 - pair, :, :, at, :],
            send_sem=pair_send.at[par],
            recv_sem=pair_recv.at[par, sem],
            device_id={"gz": pair_peer},
            device_id_type=MESH,
        )

    def from_argument(direction, start, size, h, send_sem, recv_sem, peer):
        pltpu.make_async_remote_copy(
            src_ref=now.at[:, direction, pl.ds(start, size), pl.ds(h * LANES, LANES)],
            dst_ref=halo.at[0, 1 - direction, :, h, pl.ds(PAD + start, size), :],
            send_sem=send_sem,
            recv_sem=recv_sem,
            device_id={"gz": peer},
            device_id_type=MESH,
        ).start()

    def first_send(j, carry):
        for h in range(2):
            from_argument(
                link, *link_rows(j), h, link_send.at[0], link_recv.at[0, j], link_peer
            )
        return carry

    around = jnp.logical_and(linked, lax.rem(me + core, 8) == 0)

    @pl.when(jnp.logical_and(linked, jnp.logical_not(around)))
    def _():
        lax.fori_loop(0, last, first_send, 0)
        first_send(last, 0)

    @pl.when(around)
    def _():
        loaded(field.at[0, :, :, :, inner, :], 0)

        def loaded_send(j, carry):
            over_link(0, *link_rows(j), j).start()
            return carry

        lax.fori_loop(0, last, loaded_send, 0)
        over_link(0, *link_rows(last), last).start()

    for i in range(2):
        for h in range(2):
            from_argument(
                pair, *pair_rows(i), h, pair_send.at[0], pair_recv.at[0, i], pair_peer
            )
    wave_copy = pltpu.make_async_copy(wave, wavelet, load_sem.at[3])
    wave_copy.start()
    load(lame, lambda h: first_coef.at[:, h], 1)
    load(shear, lambda h: second_coef.at[:, h], 1)
    load(density, lambda h: density_of.at[:, h], 1)
    load(prior, lambda h: prior_of.at[:, h], 1)
    load(source, lambda h: force.at[:, :, h], 1)
    load(before, lambda h: field.at[1, :, :, h, inner, :], 2)

    def send_link(par, j):
        pl.when(linked)(lambda: over_link(par, *link_rows(j), j).start())

    def send_pair(par, i):
        to_pair(par, *pair_rows(i), i).start()

    def wait_sent(par):
        to_pair(par, 0, nx, 0).wait_send()
        pl.when(linked)(lambda: over_link(par, 0, nx, 0).wait_send())

    def wait_link(par, j):
        @pl.when(linked)
        def _():
            start, size = link_rows(j)
            at = pl.ds(PAD + start, size)
            pltpu.make_async_remote_copy(
                src_ref=field.at[par, :, link, :, at, :],
                dst_ref=halo.at[par, link, :, :, at, :],
                send_sem=link_send.at[par],
                recv_sem=link_recv.at[par, j],
                device_id={"gz": link_peer},
                device_id_type=MESH,
            ).wait_recv()

    def wait_pair(par, i):
        start, size = pair_rows(i)
        at = pl.ds(PAD + start, size)
        pltpu.make_async_remote_copy(
            src_ref=field.at[par, :, pair, :, at, :],
            dst_ref=halo.at[par, pair, :, :, at, :],
            send_sem=pair_send.at[par],
            recv_sem=pair_recv.at[par, i],
            device_id={"gz": pair_peer},
            device_id_type=MESH,
        ).wait_recv()

    rounds = []
    while 4 << len(rounds) < count:
        rounds.append(4 << len(rounds))

    def far(r, d):
        return me + rounds[r] if d else me - rounds[r]

    def within(r, d):
        return far(r, d) < count if d else far(r, d) >= 0

    def tell_far(r):
        for d in range(2):

            @pl.when(within(r, d))
            def _():
                pl.semaphore_signal(
                    hello_sem.at[r], inc=1, device_id={"gz": far(r, d)}, device_id_type=MESH
                )

    def hear_far(r):
        heard = jnp.where(within(r, 0), 1, 0) + jnp.where(within(r, 1), 1, 0)
        pl.when(heard > 0)(lambda: pl.semaphore_wait(hello_sem.at[r], heard))

    def acquaint(n):
        for r in range(len(rounds) + 1):

            @pl.when(n == 3 + r)
            def _():
                if r > 0:
                    hear_far(r - 1)
                if r < len(rounds):
                    tell_far(r)


    wave_copy.wait()
    loaded(bank, 1)
    pl.when(jnp.logical_not(around))(lambda: loaded(field.at[0, :, :, :, inner, :], 0))
    loaded(field.at[1, :, :, :, inner, :], 2)
    load(steps, lambda h: s_vec.at[:, :, h], 4)
    load(changes, lambda h: y_vec.at[:, :, h], 5)

    def prepare(i, carry):
        at = pl.ds(pl.multiple_of(i * 8, 8), 8)
        for p in range(2):
            for h in range(2):
                mu = second_coef[p, h, at, :]
                coeff = 0.04 / density_of[p, h, at, :]
                first_coef[p, h, at, :] = 0.25 * coeff * (first_coef[p, h, at, :] + mu)
                second_coef[p, h, at, :] = coeff * mu
                grad[p, h, at, :] = mu - prior_of[p, h, at, :]
                for c in range(3):
                    force[c, p, h, at, :] = coeff * force[c, p, h, at, :]
        return carry

    lax.fori_loop(0, nx // 8, prepare, 0)

    for w in range(len(WANTED)):
        products[w] = zero

    def gram(bases):
        for w, (kind, a, b) in enumerate(WANTED):
            part = products[w]
            for base in bases:
                at = pl.ds(base, 8)
                for p in range(2):
                    for h in range(2):
                        one = s_vec if kind == "sy" else y_vec
                        part = part + one[a, p, h, at, :] * y_vec[b, p, h, at, :]
            products[w] = part

    def lanes_of(x, first):
        n = x.shape[0]
        sums = jnp.sum(jnp.sum(x, axis=1), axis=1, keepdims=True)
        there = lax.broadcasted_iota(jnp.int32, (n, LANES), 1)
        wanted = lax.broadcasted_iota(jnp.int32, (n, LANES), 0) + first
        return jnp.sum(jnp.where(there == wanted, sums, 0.0), axis=0, keepdims=True)

    def along_y(v):
        back = [pltpu.roll(x, 1, 1) for x in v]
        ahead = [pltpu.roll(x, LANES - 1, 1) for x in v]
        plus = (jnp.where(at_end, ahead[1], ahead[0]), jnp.where(at_end, 0.0, ahead[1]))
        minus = (jnp.where(at_start, 0.0, back[0]), jnp.where(at_start, back[0], back[1]))
        return plus, minus

    def add(a, b):
        return (a[0] + b[0], a[1] + b[1])

    def sub(a, b):
        return (a[0] - b[0], a[1] - b[1])

    def block(cur, nxt, amplitude, base, out=None):
        at = pl.ds(base, 8)

        def rows_of(c, z, offset):
            from_row = pl.ds(base + PAD + offset, 8)
            if z in (-1, 2):
                return tuple(halo[cur, 0 if z < 0 else 1, c, h, from_row, :] for h in range(2))
            return tuple(field[cur, c, z, h, from_row, :] for h in range(2))

        u = {(c, z): rows_of(c, z, 0) for c in range(3) for z in (-1, 0, 1, 2)}
        up = {}
        down = {}
        for c in range(3):
            for z in (-1, 0, 1, 2) if c < 2 else (0, 1):
                up[c, z] = rows_of(c, z, 1)
                down[c, z] = rows_of(c, z, -1)
        dx = {key: sub(up[key], down[key]) for key in up}
        dy2 = {}
        sy = {}
        for z in (-1, 0, 1, 2):
            plus, minus = along_y(u[2, z])
            dy2[z] = sub(plus, minus)
            if z in (0, 1):
                sy[2, z] = add(plus, minus)
        mix0 = {z: add(dx[1, z], dy2[z]) for z in (-1, 0, 1, 2)}
        grads = []
        for z in range(2):
            for c in range(2):
                sy[c, z] = add(*along_y(u[c, z]))
            dz0 = sub(u[0, z + 1], u[0, z - 1])
            cross = [
                sub(mix0[z + 1], mix0[z - 1]),
                add(sub(dx[0, z + 1], dx[0, z - 1]), sub(*along_y(dx[2, z]))),
                sub(*along_y(add(dz0, dx[1, z]))),
            ]
            work = [None, None]
            for c in range(3):
                sz = add(u[c, z + 1], u[c, z - 1])
                sx = add(up[c, z], down[c, z])
                own = (sz, sx, sy[c, z])[c]
                for h in range(2):
                    centre = u[c, z][h]
                    twice = centre + centre
                    laplace = sz[h] + sx[h] + sy[c, z][h] - 6.0 * centre
                    div = 4.0 * (own[h] - twice) + cross[c][h]
                    new = (
                        twice
                        - field[nxt, c, z, h, pl.ds(base + PAD, 8), :]
                        + first_coef[z, h, at, :] * div
                        + second_coef[z, h, at, :] * laplace
                        + amplitude * force[c, z, h, at, :]
                    )
                    if out is None:
                        field[nxt, c, z, h, pl.ds(base + PAD, 8), :] = new
                    else:
                        out[c, z, h, at, :] = new
                    term = centre * laplace
                    work[h] = term if work[h] is None else work[h] + term
            for h in range(2):
                new = grad[z, h, at, :] + 0.02 * work[h]
                grad[z, h, at, :] = new
                grads.append((z, h, new))
        return grads

    def sweep(cur, nxt, amplitude, out, after, ending, carry):
        def at_split(j, act):
            if isinstance(j, int):
                if j == split:
                    act()
            else:
                pl.when(j == split)(act)

        def part(j, bases, carry):
            wait_link(cur, j)
            at_split(j, lambda: wait_pair(cur, 1))
            for i, base in enumerate(bases):
                carry = after(base, block(cur, nxt, amplitude, base, out), carry)
                if i == 0 and out is None and not (isinstance(j, int) and j == 0):
                    send_link(nxt, j - 1)
                    at_split(j, lambda: send_pair(nxt, 0))
            ending(bases)
            return carry

        def later(j, carry):
            return part(j, [pl.multiple_of(j * ROWS + k, 8) for k in range(-8, ROWS - 8, 8)], carry)

        wait_pair(cur, 0)
        carry = part(0, list(range(0, ROWS - 8, 8)), carry)
        carry = lax.fori_loop(1, last, later, carry)
        carry = part(last, [last * ROWS + k for k in range(-8, REST, 8)], carry)
        if out is None:
            send_link(nxt, last)
            send_pair(nxt, 1)
        return carry

    def step(n, carry):
        cur = lax.rem(n, 2)
        nxt = 1 - cur
        pl.when(n >= 1)(lambda: wait_sent(nxt))
        acquaint(n)

        @pl.when(n == 1)
        def _():
            loaded(s_vec, 4)
            loaded(y_vec, 5)

        @pl.when(n == 2)
        def _():
            row[...] = lanes_of(products[...], 2 * PAIRS)

        return sweep(
            cur,
            nxt,
            wavelet[n],
            None,
            lambda base, grads, carry: carry,
            lambda bases: pl.when(n == 1)(lambda: gram(bases)),
            carry,
        )

    lax.fori_loop(0, STEPS - 1, step, 0)

    cur, nxt = (STEPS - 1) % 2, STEPS % 2

    def multiply(base, grads, sums):
        sums = list(sums)
        for z, h, g in grads:
            for k in range(PAIRS):
                sums[k] = sums[k] + s_vec[k, z, h, pl.ds(base, 8), :] * g
                sums[PAIRS + k] = sums[PAIRS + k] + y_vec[k, z, h, pl.ds(base, 8), :] * g
        return tuple(sums)

    sums = sweep(
        cur,
        nxt,
        wavelet[STEPS - 1],
        final,
        multiply,
        lambda bases: None,
        (zero,) * (2 * PAIRS),
    )

    rows[pl.ds(me, 1)] = (row[...] + lanes_of(jnp.stack(sums), 0))[None]

    for k in range(count - 1):
        pltpu.make_async_remote_copy(
            src_ref=rows.at[me],
            dst_ref=rows.at[me],
            send_sem=sum_send.at[0],
            recv_sem=sum_recv.at[0],
            device_id={"gz": k + jnp.where(me <= k, 1, 0)},
            device_id_type=MESH,
        ).start()

    others = rows.at[pl.ds(0, count - 1)]
    everyone = pltpu.make_async_remote_copy(
        src_ref=others,
        dst_ref=others,
        send_sem=sum_send.at[0],
        recv_sem=sum_recv.at[0],
        device_id={"gz": lax.rem(me + 1, count)},
        device_id_type=MESH,
    )
    everyone.wait_recv()
    total[...] = jnp.sum(rows[...], axis=0)
    everyone.wait_send()
    wait_sent(nxt)
    wait_sent(cur)


def finish(
    final, grad, s_vec, y_vec, total, out_field, out_gradient, out_direction, result, sem
):
    def store(src, dst, h, group):
        pltpu.make_async_copy(src, dst.at[..., pl.ds(h * LANES, LANES)], sem.at[group]).start()

    for h in range(2):
        store(final.at[:, :, h], out_field, h, 0)
        store(grad.at[:, h], out_gradient, h, 1)

    nx = grad.shape[2]
    lane = lax.broadcasted_iota(jnp.int32, (1, LANES), 1)
    sums = total[...]

    def value(k):
        return jnp.sum(jnp.where(lane == k, sums, 0.0), axis=1, keepdims=True)

    sg = [value(k) for k in range(PAIRS)]
    yg = [value(PAIRS + k) for k in range(PAIRS)]
    pair = {}
    for w, (kind, a, b) in enumerate(WANTED):
        pair[kind, a, b] = value(2 * PAIRS + w)
        if kind == "yy":
            pair[kind, b, a] = pair[kind, a, b]
    rho = [1.0 / pair["sy", i, i] for i in range(PAIRS)]
    alphas = [None] * PAIRS
    for i in reversed(range(PAIRS)):
        dot = sg[i]
        for j in reversed(range(i + 1, PAIRS)):
            dot = dot - alphas[j] * pair["sy", i, j]
        alphas[i] = dot * rho[i]
    gamma = pair["sy", PAIRS - 1, PAIRS - 1] / pair["yy", PAIRS - 1, PAIRS - 1]
    extra = []
    for i in range(PAIRS):
        dot = yg[i]
        for j in range(PAIRS):
            dot = dot - alphas[j] * pair["yy", i, j]
        dot = gamma * dot
        for j in range(i):
            dot = dot + extra[j] * pair["sy", j, i]
        extra.append(alphas[i] - dot * rho[i])

    def wide(x):
        return jnp.broadcast_to(x, (8, LANES))

    of_g = wide(-gamma)
    of_y = [wide(gamma * alphas[i]) for i in range(PAIRS)]
    of_s = [wide(-extra[i]) for i in range(PAIRS)]
    for p in range(2):

        def combine(i, carry):
            at = pl.ds(pl.multiple_of(i * 8, 8), 8)
            for h in range(2):
                parts = [of_g * grad[p, h, at, :], of_s[0] * s_vec[0, p, h, at, :]]
                for k in range(PAIRS):
                    parts[0] = parts[0] + of_y[k] * y_vec[k, p, h, at, :]
                    if k > 0:
                        parts[1] = parts[1] + of_s[k] * s_vec[k, p, h, at, :]
                result[p, h, at, :] = parts[0] + parts[1]
            return carry

        lax.fori_loop(0, nx // 8, combine, 0, unroll=4)
        for h in range(2):
            store(result.at[p, h], out_direction.at[p], h, 2)
    for group, out in enumerate((out_field, out_gradient, out_direction)):
        pltpu.make_async_copy(out, out, sem.at[group]).wait()


def on_device(*args):
    now = args[0]
    lame = args[2]
    nx = now.shape[2]
    count = lax.axis_size("gz")
    padded = nx + 2 * PAD
    chunks = (nx - REST) // ROWS + 1
    f32 = jnp.float32
    hbm = pl.BlockSpec(memory_space=pltpu.HBM)
    vmem = pl.BlockSpec(memory_space=pltpu.VMEM)
    in_specs = [hbm] * 10
    plane = (2, 2, nx, LANES)
    halves = pl.pallas_call(
        kernel,
        out_shape=(
            jax.ShapeDtypeStruct((3, *plane), f32),
            jax.ShapeDtypeStruct(plane, f32),
            jax.ShapeDtypeStruct((PAIRS, *plane), f32),
            jax.ShapeDtypeStruct((PAIRS, *plane), f32),
            jax.ShapeDtypeStruct((1, LANES), f32),
        ),
        in_specs=in_specs,
        out_specs=(vmem,) * 5,
        scratch_shapes=[
            pltpu.SMEM((STEPS,), f32),
            pltpu.VMEM((2, 3, 2, 2, padded, LANES), f32),
            pltpu.VMEM((2, 2, 3, 2, padded, LANES), f32),
            pltpu.VMEM((7, *plane), f32),
            pltpu.VMEM((len(WANTED), 8, LANES), f32),
            pltpu.VMEM((1, LANES), f32),
            pltpu.VMEM((count, 1, LANES), f32),
            pltpu.SemaphoreType.DMA((2,)),
            pltpu.SemaphoreType.DMA((2, chunks)),
            pltpu.SemaphoreType.DMA((2,)),
            pltpu.SemaphoreType.DMA((2, 2)),
            pltpu.SemaphoreType.DMA((6,)),
            pltpu.SemaphoreType.REGULAR((3,)),
            pltpu.SemaphoreType.DMA((1,)),
            pltpu.SemaphoreType.DMA((1,)),
        ],
        compiler_params=pltpu.CompilerParams(
            collective_id=0, has_side_effects=True, vmem_limit_bytes=20 * 1024 * 1024
        ),
        name="leapfrog",
    )(*[pltpu.with_memory_space_constraint(x, pltpu.HBM) for x in args])
    return pl.pallas_call(
        finish,
        out_shape=(
            jax.ShapeDtypeStruct(now.shape, f32),
            jax.ShapeDtypeStruct(lame.shape, f32),
            jax.ShapeDtypeStruct(lame.shape, f32),
        ),
        in_specs=[vmem] * 5,
        out_specs=(hbm,) * 3,
        scratch_shapes=[pltpu.VMEM(plane, f32), pltpu.SemaphoreType.DMA((3,))],
        compiler_params=pltpu.CompilerParams(vmem_limit_bytes=8 * 1024 * 1024),
        name="finish",
    )(*halves)


def solution(mesh):
    placed = (
        P("sample", "gz", None, None),
        P("sample", "gz", None, None),
        P("gz", "sample", None),
        P("gz", "sample", None),
        P("gz", "sample", None),
        P("sample", "gz", None, None),
        P("sample"),
        P("gz", "sample", None),
        P("sample", "gz", None, None),
        P("sample", "gz", None, None),
    )
    return jax.shard_map(
        on_device,
        mesh=mesh,
        in_specs=placed,
        out_specs=(P("sample", "gz", None, None), P("gz", "sample", None), P("gz", "sample", None)),
        check_vma=False,
    )
```
